16 devices in a mesh: tp: 2 (over z), dp: 8 (over y, x, core).
Axes of the slice: x: 2, y: 2, z: 2, core: 2. Of those that a mesh axis runs over, the one named last changes fastest.
Arguments:
- x_in: bfloat16 [4096, 2048], P('dp')
- w_gate: bfloat16 [2048, 5632], P('dp', 'tp')
- w_up: bfloat16 [2048, 5632], P('dp', 'tp')
- w_down: bfloat16 [5632, 2048], P('tp', 'dp')
- dy_in: bfloat16 [4096, 2048], P('dp')
Outputs:
- output 1: bfloat16 [4096, 2048], P('dp')
- output 2: bfloat16 [4096, 2048], P('dp')
- output 3: float32 [2048, 5632], P('dp', 'tp')
- output 4: float32 [2048, 5632], P('dp', 'tp')
- output 5: float32 [5632, 2048], P('tp', 'dp')
All inputs are finite; a program needn't handle non-finite values.
Results may differ from the reference program's by a relative error of at most 0.001.
Values are sent between devices in bfloat16 or wider.
A program may use at most 1 GiB of HBM per device.

```python
import jax
import jax.numpy as jnp
from jax import lax

MODEL_DIM = 2048
HIDDEN_DIM = 5632
SHARD_TOKENS = 512
DATA_SHARDS = 8


def setup_inputs(seed: int = 0) -> dict:
    key_list = jax.random.split(jax.random.key(seed), 5)
    row_count = DATA_SHARDS * SHARD_TOKENS
    x_vals = jax.random.normal(key_list[0], (row_count, MODEL_DIM), jnp.float32)
    gate_vals = jax.random.normal(key_list[1], (MODEL_DIM, HIDDEN_DIM), jnp.float32) * MODEL_DIM ** -0.5
    up_vals = jax.random.normal(key_list[2], (MODEL_DIM, HIDDEN_DIM), jnp.float32) * MODEL_DIM ** -0.5
    down_vals = jax.random.normal(key_list[3], (HIDDEN_DIM, MODEL_DIM), jnp.float32) * HIDDEN_DIM ** -0.5
    dy_vals = jax.random.normal(key_list[4], (row_count, MODEL_DIM), jnp.float32)
    return {
        'x_in': x_vals.astype(jnp.bfloat16),
        'w_gate': gate_vals.astype(jnp.bfloat16),
        'w_up': up_vals.astype(jnp.bfloat16),
        'w_down': down_vals.astype(jnp.bfloat16),
        'dy_in': dy_vals.astype(jnp.bfloat16),
    }


def reference(x_in, w_gate, w_up, w_down, dy_in):
    row_count = DATA_SHARDS * SHARD_TOKENS
    x_blocks = x_in.reshape(DATA_SHARDS, SHARD_TOKENS, MODEL_DIM)
    dy_blocks = dy_in.reshape(DATA_SHARDS, SHARD_TOKENS, MODEL_DIM)

    def shard_pass(carry, block):
        acc_gate, acc_up, acc_down = carry
        x_blk, dy_blk = block
        gate_pre = jnp.dot(x_blk, w_gate, preferred_element_type=jnp.float32)
        up_pre = jnp.dot(x_blk, w_up, preferred_element_type=jnp.float32)
        sig_gate = jax.nn.sigmoid(gate_pre)
        silu_gate = gate_pre * sig_gate
        hidden = (silu_gate * up_pre).astype(jnp.bfloat16)
        y_blk = (x_blk.astype(jnp.float32) + jnp.dot(hidden, w_down, preferred_element_type=jnp.float32)).astype(jnp.bfloat16)
        grad_h = jnp.dot(dy_blk, w_down.T, preferred_element_type=jnp.float32)
        d_gate = (grad_h * up_pre * sig_gate * (1.0 + gate_pre * (1.0 - sig_gate))).astype(jnp.bfloat16)
        d_up = (grad_h * silu_gate).astype(jnp.bfloat16)
        dx_blk = (dy_blk.astype(jnp.float32)
                  + jnp.dot(d_gate, w_gate.T, preferred_element_type=jnp.float32)
                  + jnp.dot(d_up, w_up.T, preferred_element_type=jnp.float32)).astype(jnp.bfloat16)
        acc_gate = acc_gate + jnp.dot(x_blk.T, d_gate, preferred_element_type=jnp.float32)
        acc_up = acc_up + jnp.dot(x_blk.T, d_up, preferred_element_type=jnp.float32)
        acc_down = acc_down + jnp.dot(hidden.T, dy_blk, preferred_element_type=jnp.float32)
        return (acc_gate, acc_up, acc_down), (y_blk, dx_blk)

    zero_acc = (jnp.zeros((MODEL_DIM, HIDDEN_DIM), jnp.float32),
                jnp.zeros((MODEL_DIM, HIDDEN_DIM), jnp.float32),
                jnp.zeros((HIDDEN_DIM, MODEL_DIM), jnp.float32))
    sums, outs = lax.scan(shard_pass, zero_acc, (x_blocks, dy_blocks))
    y_blocks, dx_blocks = outs
    return (y_blocks.reshape(row_count, MODEL_DIM), dx_blocks.reshape(row_count, MODEL_DIM), sums[0], sums[1], sums[2])
```

```python
import functools

import jax
import jax.numpy as jnp
from jax import lax
from jax.experimental import pallas as pl
from jax.experimental.pallas import tpu as pltpu
from jax.sharding import PartitionSpec as P

MESH = pl.DeviceIdType.MESH
BF16, F32 = jnp.bfloat16, jnp.float32
D, FH, FQ, ROWS, TOK = 2048, 2816, 1408, 256, 512
SUB = 256
NN = (((1,), (0,)), ((), ()))
NT = (((1,), (1,)), ((), ()))


def dot(a, b, dims):
    return lax.dot_general(a, b, dims, preferred_element_type=F32)


def kernel(x_in, wg_in, wu_in, wd_in, dy_in,
           y_out, dx_out, dwg_out, dwu_out, dwd_out, x_all, dy_all,
           wg, wu, wd, acc, xb, dyb, hb, dab, dbb, pb, rc, rz, fb, xt, dyt,
           wl, ws, wr, xl, xs, xf, xd, xr, pr, cs, cr, zs, zr, bs, br, fl, ds, dr, dl):
    tp, dp = lax.axis_index('tp'), lax.axis_index('dp')
    core, xc, yc = lax.rem(dp, 2), lax.rem(lax.div(dp, 2), 2), lax.div(dp, 4)
    col = lax.div(dp, 2)

    def idx(yy, xx, cc):
        return yy * 4 + xx * 2 + cc

    def dev(yy, xx, cc):
        return (tp, idx(yy, xx, cc))

    partner = dev(yc, xc, 1 - core)
    zdev = (1 - tp, dp)

    barrier = pltpu.get_barrier_semaphore()
    peers = [partner, zdev] + [dev(yc, 1 - xc, cc) for cc in (0, 1)] + [dev(1 - yc, xc, cc) for cc in (0, 1)]
    for peer in peers:
        pl.semaphore_signal(barrier, inc=1, device_id=peer, device_id_type=MESH)
    pl.semaphore_wait(barrier, len(peers))

    def remote(src, dst, ssem, rsem, device):
        return pltpu.make_async_remote_copy(src_ref=src, dst_ref=dst, send_sem=ssem, recv_sem=rsem,
                                            device_id=device, device_id_type=MESH)

    def w_src(m, cc):
        if m == 2:
            return wd_in.at[pl.ds(pl.multiple_of(cc * FQ, 128), FQ), :]
        return (wg_in, wu_in)[m].at[:, pl.ds(pl.multiple_of(cc * FQ, 128), FQ)]

    def w_at(m, r):
        if m == 2:
            return wd.at[r]
        return (wg, wu)[m].at[pl.ds(pl.multiple_of(r * ROWS, ROWS), ROWS), :]

    def w_local(m):
        return pltpu.make_async_copy(w_src(m, core), w_at(m, dp), wl.at[m])

    def w_direct(m):
        out = [remote(w_src(m, 1 - core), w_at(m, dp), ws.at[m, 0], wr.at[m, 0], partner)]
        for cc in (0, 1):
            out.append(remote(w_src(m, cc), w_at(m, dp), ws.at[m, 1 + cc], wr.at[m, 1 + core], dev(yc, 1 - xc, cc)))
            out.append(remote(w_src(m, cc), w_at(m, dp), ws.at[m, 3 + cc], wr.at[m, 3 + core], dev(1 - yc, xc, cc)))
        return out

    rx, ry = idx(yc, 1 - xc, 0), idx(1 - yc, xc, 1)

    def w_forward(m):
        return [remote(w_at(m, rx), w_at(m, rx), ws.at[m, 5], wr.at[m, 5], dev(1 - yc, xc, core)),
                remote(w_at(m, ry), w_at(m, ry), ws.at[m, 6], wr.at[m, 6], dev(yc, 1 - xc, core))]

    def w_wait(m, slot):
        remote(w_at(m, dp), w_at(m, dp), ws.at[m, slot], wr.at[m, slot], partner).wait_recv()

    arrays = ((x_in, x_all, xb), (dy_in, dy_all, dyb))

    def rows(j):
        return pl.ds(pl.multiple_of(j * SUB, SUB), SUB)

    def t_at(a, rel, s, j):
        return arrays[a][1].at[rel * 2 + s, rows(j)]

    def t_own(a, j, k):
        src = arrays[a][0].at[rows(j)]
        rel = (1, 2, 0)[k]
        sem = pr.at[0, j, a] if k == 2 else xr.at[rel, j, a]
        return remote(src, t_at(a, rel, core, j), xs.at[j, a, k], sem,
                      (dev(yc, 1 - xc, core), dev(1 - yc, xc, core), partner)[k])

    def t_share(a, rel, j):
        return remote(t_at(a, rel, core, j), t_at(a, rel, core, j), xd.at[rel, j, a], pr.at[rel, j, a], partner)

    fwd_dev = dev(yc + (1 - core) * (1 - 2 * yc), xc + core * (1 - 2 * xc), core)

    def t_forward(a, j):
        return remote(t_at(a, 1 + core, core, j), t_at(a, 3, core, j), xf.at[j, a], xr.at[3, j, a], fwd_dev)

    def t_wait_own(a, rel, j):
        remote(t_at(a, rel, core, j), t_at(a, rel, core, j), xd.at[rel, j, a], xr.at[rel, j, a], partner).wait_recv()

    def t_load(a, rel, s, j):
        half = 0 if s == 'own' else 1
        source = core if s == 'own' else 1 - core
        return pltpu.make_async_copy(t_at(a, rel, source, j), arrays[a][2].at[pl.ds(half * SUB, SUB)], xl.at[half, a])

    def t_load_own(a, j):
        return pltpu.make_async_copy(arrays[a][0].at[rows(j)], arrays[a][2].at[pl.ds(0, SUB)], xl.at[0, a])

    def gates(a, b, g):
        s = jax.nn.sigmoid(a)
        silu = a * s
        return ((silu * b).astype(BF16), (g * b * s * (1.0 + a * (1.0 - s))).astype(BF16), (g * silu).astype(BF16))

    def tiles(body):
        def step(n, carry):
            body(pl.ds(pl.multiple_of(n * 256, 256), 256))
            return carry
        lax.fori_loop(0, FQ // 256, step, 0)
        body(pl.ds(FQ // 256 * 256, FQ % 256))

    def grad_tile(r, cols):
        g = dot(dyb[r, 0:ROWS], wd[0, cols, :], NT)
        for i in range(1, 8):
            g = g + dot(dyb[r, i * ROWS:(i + 1) * ROWS], wd[i, cols, :], NT)
        return g

    def phase1(r):
        def body(cols):
            a = dot(xb[r, :], wg[:, cols], NN)
            b = dot(xb[r, :], wu[:, cols], NN)
            g = grad_tile(r, cols)
            hb[r, cols], dab[r, cols], dbb[r, cols] = gates(a, b, g)
        tiles(body)

    def weight_grads(r, size):
        own_cols = pl.ds(pl.multiple_of(col * 512, 512), 512)
        xt[:, 0:size] = xb[r, own_cols].T
        dyt[:, 0:size] = dyb[r, own_cols].T

        def body(cols):
            acc[0, :, cols] += dot(xt[:, 0:size], dab[r, cols], NN)
            acc[1, :, cols] += dot(xt[:, 0:size], dbb[r, cols], NN)
            acc[2, :, cols] += dot(dyt[:, 0:size], hb[r, cols], NN)
        tiles(body)

    def partial_out():
        def step(i, carry):
            cols = pl.ds(pl.multiple_of(i * ROWS, ROWS), ROWS)
            pb[0, :, cols] = dot(hb[...], wd[i], NN)
            pb[1, :, cols] = dot(dab[...], wg[cols, :], NT) + dot(dbb[...], wu[cols, :], NT)
            return carry
        lax.fori_loop(0, 8, step, 0)

    def c_send(p, a):
        return remote(pb.at[a, pl.ds(SUB, SUB)], rc.at[p, a], cs.at[p, a], cr.at[p, a], partner)

    def z_send(p, a):
        return remote(rc.at[p, a, pl.ds(pl.multiple_of((1 - tp) * 128, 128), 128)], rz.at[p, a],
                      zs.at[p, a], zr.at[p, a], zdev)

    outs = (y_out, dx_out)

    def out_rows(p, half):
        return pl.ds(pl.multiple_of(p * SUB + half * 128, 128), 128)

    def b_send(p, a):
        return remote(fb.at[p, a], outs[a].at[out_rows(p, tp)], bs.at[p, a], br.at[p, a], zdev)

    def b_local(p, a):
        return pltpu.make_async_copy(fb.at[p, a], outs[a].at[out_rows(p, tp)], fl.at[p, a])

    def c_reduce(p):
        src = (xb, dyb)
        for a in (0, 1):
            c_send(p, a).wait_recv()
            def step(i, carry):
                rr = pl.ds(pl.multiple_of(i * 32, 32), 32)
                rc[p, a, rr, :] = rc[p, a, rr, :] + pb[a, rr, :]
                return carry
            lax.fori_loop(0, SUB // 32, step, 0)
            z_send(p, a).start()
            keep = pl.multiple_of(tp * 128, 128)
            def step2(i, carry):
                rr = pl.ds(pl.multiple_of(keep + i * 32, 32), 32)
                rc[p, a, rr, :] = rc[p, a, rr, :] + src[a][rr, :].astype(F32)
                return carry
            lax.fori_loop(0, 4, step2, 0)

    def finalize(p, a):
        z_send(p, a).wait_recv()
        keep = pl.multiple_of(tp * 128, 128)
        def step(i, carry):
            rr = pl.ds(pl.multiple_of(i * 32, 32), 32)
            kr = pl.ds(pl.multiple_of(keep + i * 32, 32), 32)
            fb[p, a, rr, :] = (rc[p, a, kr, :] + rz[p, a, rr, :]).astype(BF16)
            return carry
        lax.fori_loop(0, 4, step, 0)
        b_send(p, a).start()
        b_local(p, a).start()

    for m in (0, 1, 2):
        w_local(m).start()
    for m in (0, 1):
        for c in w_direct(m):
            c.start()
    for j in (0, 1):
        for a in (0, 1):
            t_own(a, j, 2).start()
    for a in (0, 1):
        t_load_own(a, 0).start()

    def zero(i, carry):
        acc[:, pl.ds(pl.multiple_of(i * 32, 32), 32), :] = jnp.zeros((3, 32, FQ), F32)
        return carry
    lax.fori_loop(0, 16, zero, 0)

    for m in (0, 1):
        w_wait(m, 1)
        w_wait(m, 4)
        for c in w_forward(m):
            c.start()
    for c in w_direct(2):
        c.start()

    for a in (0, 1):
        t_own(a, 0, 2).wait_recv()
        t_load(a, 0, 'partner', 0).start()
    for m in (0, 1):
        w_local(m).wait()
        for slot in (0, 2, 3, 5, 6):
            w_wait(m, slot)
    for half in (0, 1):
        pltpu.make_async_copy(x_in.at[rows(0)], xb.at[pl.ds(half * SUB, SUB)], xl.at[half, 0]).wait()
        pltpu.make_async_copy(x_in.at[rows(0)], dyb.at[pl.ds(half * SUB, SUB)], xl.at[half, 1]).wait()

    everything = pl.ds(0, 2 * SUB)

    def early(cols):
        a = dot(xb[...], wg[:, cols], NN)
        b = dot(xb[...], wu[:, cols], NN)
        pb[0, :, cols], pb[1, :, cols] = a, b
    tiles(early)

    w_wait(2, 1)
    w_wait(2, 4)
    for c in w_forward(2):
        c.start()
    for j in (0, 1):
        for a in (0, 1):
            for k in (0, 1):
                t_own(a, j, k).start()
    w_local(2).wait()
    for slot in (0, 2, 3, 5, 6):
        w_wait(2, slot)

    def late(cols):
        g = grad_tile(everything, cols)
        hb[:, cols], dab[:, cols], dbb[:, cols] = gates(pb[0, :, cols], pb[1, :, cols], g)
    tiles(late)
    partial_out()
    for a in (0, 1):
        c_send(0, a).start()
    weight_grads(everything, 512)
    c_reduce(0)

    for a in (0, 1):
        t_load_own(a, 1).start()
        t_own(a, 1, 2).wait_recv()
        t_load(a, 0, 'partner', 1).start()
    for a in (0, 1):
        for half in (0, 1):
            pltpu.make_async_copy(x_in.at[rows(0)], arrays[a][2].at[pl.ds(half * SUB, SUB)], xl.at[half, a]).wait()
    phase1(everything)
    for a in (0, 1):
        c_send(0, a).wait_send()
    partial_out()
    for a in (0, 1):
        c_send(1, a).start()
    weight_grads(everything, 512)
    c_reduce(1)

    def block(k):
        first = (k + 2) // 2
        mid = (first * (3 - first)) // 2
        e = lax.rem(k, 2)
        return mid * (1 + e) + (1 - mid) * first, mid * (first - 1) + (1 - mid) * e

    def service(k):
        rel, j = block(k)
        for a in (0, 1):
            t_wait_own(a, rel, j)
            t_share(a, rel, j).start()
            t_load(a, rel, 'own', j).start()
        @pl.when(rel == 1 + core)
        def _():
            for a in (0, 1):
                t_forward(a, j).start()

    service(jnp.int32(0))

    def unit(t, carry):
        k, s = lax.div(t, 2), lax.rem(t, 2)

        @pl.when(s == 0)
        def _():
            rel, j = block(k)
            for a in (0, 1):
                t_share(a, rel, j).wait_recv()
                t_load(a, rel, 'partner', j).start()

        @pl.when(jnp.logical_and(s == 1, k < 5))
        def _():
            service(k + 1)

        for a in (0, 1):
            pltpu.make_async_copy(x_in.at[rows(0)], arrays[a][2].at[pl.ds(pl.multiple_of(s * SUB, SUB), SUB)],
                                  xl.at[s, a]).wait()
        r = pl.ds(pl.multiple_of(s * SUB, SUB), SUB)
        phase1(r)
        weight_grads(r, SUB)

        for q in range(4):
            @pl.when(t == 2 * q + 2)
            def _():
                finalize(q // 2, q % 2)
        return carry
    lax.fori_loop(0, 12, unit, 0)

    grads = (dwg_out, dwu_out, dwd_out)

    def g_part(n, c):
        return acc.at[n, pl.ds(pl.multiple_of(c * ROWS, ROWS), ROWS), :]

    def g_at(n):
        return grads[n].at[:, pl.ds(pl.multiple_of(core * FQ, 128), FQ)]

    g_send = [remote(g_part(n, 1 - core), g_at(n), ds.at[n], dr.at[n], partner) for n in range(3)]
    g_local = [pltpu.make_async_copy(g_part(n, core), g_at(n), dl.at[n]) for n in range(3)]
    for n in range(3):
        g_send[n].start()
        g_local[n].start()

    for m in (0, 1, 2):
        for c in w_direct(m) + w_forward(m):
            c.wait_send()
    for a in (0, 1):
        for j in (0, 1):
            for k in (0, 1, 2):
                t_own(a, j, k).wait_send()
            t_forward(a, j).wait_send()
            for rel in (1, 2, 3):
                t_share(a, rel, j).wait_send()
        c_send(1, a).wait_send()
        for p in (0, 1):
            z_send(p, a).wait_send()
            b_local(p, a).wait()
            b_send(p, a).wait()
    for n in range(3):
        g_local[n].wait()
        g_send[n].wait()


def solution(mesh):
    sds = jax.ShapeDtypeStruct
    dma, vmem = pltpu.SemaphoreType.DMA, pltpu.VMEM

    def device_pass(x, wg, wu, wd, dy):
        anyspec = pl.BlockSpec(memory_space=pl.ANY)
        out = pl.pallas_call(
            kernel,
            out_shape=[sds((TOK, D), BF16), sds((TOK, D), BF16), sds((ROWS, FH), F32), sds((ROWS, FH), F32),
                       sds((ROWS, FH), F32), sds((8, TOK, D), BF16), sds((8, TOK, D), BF16)],
            in_specs=[anyspec] * 5,
            out_specs=[anyspec] * 7,
            scratch_shapes=[
                vmem((D, FQ), BF16), vmem((D, FQ), BF16), vmem((8, FQ, ROWS), BF16),
                vmem((3, 512, FQ), F32),
                vmem((2 * SUB, D), BF16), vmem((2 * SUB, D), BF16),
                vmem((2 * SUB, FQ), BF16), vmem((2 * SUB, FQ), BF16), vmem((2 * SUB, FQ), BF16),
                vmem((2, 2 * SUB, D), F32), vmem((2, 2, SUB, D), F32), vmem((2, 2, 128, D), F32),
                vmem((2, 2, 128, D), BF16),
                vmem((512, 2 * SUB), BF16), vmem((512, 2 * SUB), BF16),
                dma((3,)), dma((3, 7)), dma((3, 7)),
                dma((2, 2)), dma((2, 2, 3)), dma((2, 2)), dma((4, 2, 2)), dma((4, 2, 2)), dma((4, 2, 2)),
                dma((2, 2)), dma((2, 2)), dma((2, 2)), dma((2, 2)), dma((2, 2)), dma((2, 2)), dma((2, 2)),
                dma((3,)), dma((3,)), dma((3,)),
            ],
            compiler_params=pltpu.CompilerParams(collective_id=0, has_side_effects=True,
                                                 vmem_limit_bytes=67043328),
        )(x, wg, wu, wd, dy)
        return out[0], out[1], out[2], out[3], out[4].T

    row_spec = P('dp', None)
    weight_spec = P('dp', 'tp')
    down_spec = P('tp', 'dp')
    return jax.shard_map(device_pass, mesh=mesh,
                         in_specs=(row_spec, weight_spec, weight_spec, down_spec, row_spec),
                         out_specs=(row_spec, row_spec, weight_spec, weight_spec, down_spec),
                         check_vma=False)
```

```python
import functools

import jax
import jax.numpy as jnp
from jax import lax
from jax.experimental import pallas as pl
from jax.experimental.pallas import tpu as pltpu
from jax.sharding import PartitionSpec as P

MESH = pl.DeviceIdType.MESH
BF16, F32 = jnp.bfloat16, jnp.float32
D, FH, FQ, ROWS, TOK = 2048, 2816, 1408, 256, 512
SUB, BLK, PIECES = 128, 256, 4
NN = (((1,), (0,)), ((), ()))
NT = (((1,), (1,)), ((), ()))


def dot(a, b, dims):
    return lax.dot_general(a, b, dims, preferred_element_type=F32)


def kernel(x_in, wg_in, wu_in, wd_in, dy_in,
           y_out, dx_out, dwg_out, dwu_out, dwd_out, x_all, dy_all,
           wg, wu, wd, acc, xb, dyb, hb, dab, dbb, pb, rc, rz, fb, xt, dyt,
           wl, ws, wr, xl, os, orr, xs, xf, xd, xr, pr, ys, yr, vs, vr, cs, cr, zs, zr, bs, br, fl, ds, dr, dl):
    tp, dp = lax.axis_index('tp'), lax.axis_index('dp')
    core, xc, yc = lax.rem(dp, 2), lax.rem(lax.div(dp, 2), 2), lax.div(dp, 4)
    col = lax.div(dp, 2)

    def idx(yy, xx, cc):
        return yy * 4 + xx * 2 + cc

    def dev(yy, xx, cc):
        return (tp, idx(yy, xx, cc))

    partner = dev(yc, xc, 1 - core)
    zdev = (1 - tp, dp)

    barrier = pltpu.get_barrier_semaphore()
    peers = [partner, zdev] + [dev(yc, 1 - xc, cc) for cc in (0, 1)] + [dev(1 - yc, xc, cc) for cc in (0, 1)]
    for peer in peers:
        pl.semaphore_signal(barrier, inc=1, device_id=peer, device_id_type=MESH)
    pl.semaphore_wait(barrier, len(peers))

    def remote(src, dst, ssem, rsem, device):
        return pltpu.make_async_remote_copy(src_ref=src, dst_ref=dst, send_sem=ssem, recv_sem=rsem,
                                            device_id=device, device_id_type=MESH)

    def w_src(m, cc):
        if m == 2:
            return wd_in.at[pl.ds(pl.multiple_of(cc * FQ, 128), FQ), :]
        return (wg_in, wu_in)[m].at[:, pl.ds(pl.multiple_of(cc * FQ, 128), FQ)]

    def w_at(m, r):
        if m == 2:
            return wd.at[r]
        return (wg, wu)[m].at[pl.ds(pl.multiple_of(r * ROWS, ROWS), ROWS), :]

    def w_local(m):
        return pltpu.make_async_copy(w_src(m, core), w_at(m, dp), wl.at[m])

    def w_direct(m):
        out = [remote(w_src(m, 1 - core), w_at(m, dp), ws.at[m, 0], wr.at[m, 0], partner)]
        for cc in (0, 1):
            out.append(remote(w_src(m, cc), w_at(m, dp), ws.at[m, 1 + cc], wr.at[m, 1 + core], dev(yc, 1 - xc, cc)))
            out.append(remote(w_src(m, cc), w_at(m, dp), ws.at[m, 3 + cc], wr.at[m, 3 + core], dev(1 - yc, xc, cc)))
        return out

    rx, ry = idx(yc, 1 - xc, 0), idx(1 - yc, xc, 1)

    def w_forward(m):
        return [remote(w_at(m, rx), w_at(m, rx), ws.at[m, 5], wr.at[m, 5], dev(1 - yc, xc, core)),
                remote(w_at(m, ry), w_at(m, ry), ws.at[m, 6], wr.at[m, 6], dev(yc, 1 - xc, core))]

    def w_wait(m, slot):
        remote(w_at(m, dp), w_at(m, dp), ws.at[m, slot], wr.at[m, slot], partner).wait_recv()

    arrays = ((x_in, x_all), (dy_in, dy_all))

    def rows(j, size=SUB):
        return pl.ds(pl.multiple_of(j * size, size), size)

    def t_at(a, rel, s, j):
        return arrays[a][1].at[rel * 2 + s, rows(j)]

    def t_partner(a, p):
        return remote(arrays[a][0].at[rows(p, BLK)], arrays[a][1].at[core, rows(p, BLK)],
                      os.at[p, a], orr.at[p, a], partner)

    def t_own(a, j, k):
        return remote(arrays[a][0].at[rows(j)], t_at(a, 1 + k, core, j), xs.at[j, a, k], xr.at[1 + k, j, a],
                      (dev(yc, 1 - xc, core), dev(1 - yc, xc, core))[k])

    def t_share(a, rel, j):
        return remote(t_at(a, rel, core, j), t_at(a, rel, core, j), xd.at[rel, j, a], pr.at[rel, j, a], partner)

    fwd_dev = dev(yc + (1 - core) * (1 - 2 * yc), xc + core * (1 - 2 * xc), core)

    def t_forward(a, j):
        return remote(t_at(a, 1 + core, core, j), t_at(a, 3, core, j), xf.at[j, a], xr.at[3, j, a], fwd_dev)

    def t_wait_own(a, rel, j):
        remote(t_at(a, rel, core, j), t_at(a, rel, core, j), xd.at[rel, j, a], xr.at[rel, j, a], partner).wait_recv()

    def p_loads(a, p, ref, sem):
        return [pltpu.make_async_copy(arrays[a][0].at[rows(p, BLK)], ref.at[pl.ds(0, BLK)], xl.at[sem, 0]),
                pltpu.make_async_copy(arrays[a][1].at[1 - core, rows(p, BLK)], ref.at[pl.ds(BLK, BLK)], xl.at[sem, 1])]

    bufs = (xb, dyb)

    def u_load(a, rel, j, half, slot):
        source = core if half == 0 else 1 - core
        return pltpu.make_async_copy(t_at(a, rel, source, j),
                                     bufs[a].at[pl.ds(pl.multiple_of(slot * BLK + half * SUB, SUB), SUB)],
                                     xl.at[4 + slot * 2 + half, a])

    def gates(a, b, g):
        s = jax.nn.sigmoid(a)
        silu = a * s
        return ((silu * b).astype(BF16), (g * b * s * (1.0 + a * (1.0 - s))).astype(BF16), (g * silu).astype(BF16))

    main, rest = FQ // 256, pl.ds(FQ // 256 * 256, FQ % 256)

    def tiles(body):
        def step(n, carry):
            body(pl.ds(pl.multiple_of(n * 256, 256), 256))
            return carry
        lax.fori_loop(0, main, step, 0)

    def grad_tile(dy, r, cols):
        g = dot(dy[r, 0:ROWS], wd[0, cols, :], NT)
        for i in range(1, 8):
            g = g + dot(dy[r, i * ROWS:(i + 1) * ROWS], wd[i, cols, :], NT)
        return g

    def rest_pair(x, r):
        both = dot(x[r, :], jnp.concatenate([wg[:, rest], wu[:, rest]], axis=1), NN)
        return both[:, 0:FQ % 256], both[:, FQ % 256:]

    def phase1(x, dy, r, o):
        def body(cols):
            a = dot(x[r, :], wg[:, cols], NN)
            b = dot(x[r, :], wu[:, cols], NN)
            hb[o, cols], dab[o, cols], dbb[o, cols] = gates(a, b, grad_tile(dy, r, cols))
        tiles(body)
        a, b = rest_pair(x, r)
        hb[o, rest], dab[o, rest], dbb[o, rest] = gates(a, b, grad_tile(dy, r, rest))

    def transposes(x, dy, r, size):
        own_cols = pl.ds(pl.multiple_of(col * 512, 512), 512)
        xt[:, 0:size] = x[r, own_cols].T
        dyt[:, 0:size] = dy[r, own_cols].T

    def weight_grads(size, first=False):
        o = pl.ds(0, size)

        def put(n, cols, value):
            acc[n, :, cols] = value if first else acc[n, :, cols] + value

        def body(cols):
            put(0, cols, dot(xt[:, 0:size], dab[o, cols], NN))
            put(1, cols, dot(xt[:, 0:size], dbb[o, cols], NN))
            put(2, cols, dot(dyt[:, 0:size], hb[o, cols], NN))
        tiles(body)
        both = dot(xt[:, 0:size], jnp.concatenate([dab[o, rest], dbb[o, rest]], axis=1), NN)
        put(0, rest, both[:, 0:FQ % 256])
        put(1, rest, both[:, FQ % 256:])
        put(2, rest, dot(dyt[:, 0:size], hb[o, rest], NN))

    cols_of = [pl.ds(pl.multiple_of(q * 512, 512), 512)
               for q in (col, yc * 2 + 1 - xc, (1 - yc) * 2 + xc, (1 - yc) * 2 + 1 - xc)]
    first_of = [q * 2 for q in (col, yc * 2 + 1 - xc, (1 - yc) * 2 + xc, (1 - yc) * 2 + 1 - xc)]

    def y_buf(p, rel):
        k = p * 4 + rel
        return (acc, k // 2, k % 2 * 512) if k < 6 else (pb, k - 6, FQ)

    def y_send(p, rel):
        ref, n, off = y_buf(p, rel)
        return remote(ref.at[n, pl.ds(BLK, BLK), pl.ds(off, 512)], rc.at[p, 0, :, cols_of[rel]],
                      ys.at[p, rel], yr.at[p, rel], partner)

    def y_zsend(p, rel):
        return remote(rc.at[p, 0, rows(1 - tp, 128), cols_of[rel]], rz.at[p, 0, :, cols_of[rel]],
                      vs.at[p, rel], vr.at[p, rel], zdev)

    def y_group(p, rel):
        ref, n, off = y_buf(p, rel)
        h = (hb, dbb)[p]

        def step(i, carry):
            ref[n, :, pl.ds(pl.multiple_of(off + i * ROWS, 128), ROWS)] = dot(h[...], wd[first_of[rel] + i], NN)
            return carry
        lax.fori_loop(0, 2, step, 0)
        y_send(p, rel).start()

    def add_rows(total, count, base, body):
        def step(i, carry):
            body(pl.ds(pl.multiple_of(base + i * count, count), count), i)
            return carry
        lax.fori_loop(0, total // count, step, 0)

    def y_finish(p, rel):
        ref, n, off = y_buf(p, rel)
        cols = cols_of[rel]
        y_send(p, rel).wait_recv()

        def both(rr, i):
            rc[p, 0, rr, cols] = rc[p, 0, rr, cols] + ref[n, rr, pl.ds(off, 512)]
        add_rows(BLK, 64, 0, both)
        y_zsend(p, rel).start()
        x = (xb, fb)[p]

        def keep(rr, i):
            rc[p, 0, rr, cols] = rc[p, 0, rr, cols] + x[rr, cols].astype(F32)
        add_rows(128, 64, tp * 128, keep)

    def dx_block(p):
        def step(i, carry):
            cols = pl.ds(pl.multiple_of(i * ROWS, ROWS), ROWS)
            pb[p, :, cols] = dot(dab[...], wg[cols, :], NT) + dot(dbb[...], wu[cols, :], NT)
            return carry
        lax.fori_loop(0, 8, step, 0)
        c_send(p).start()

    def c_send(p):
        return remote(pb.at[p, pl.ds(BLK, BLK)], rc.at[p, 1], cs.at[p], cr.at[p], partner)

    def z_send(p):
        return remote(rc.at[p, 1, rows(1 - tp, 128)], rz.at[p, 1], zs.at[p], zr.at[p], zdev)

    def dx_finish(p, dy):
        c_send(p).wait_recv()

        def both(rr, i):
            rc[p, 1, rr, :] = rc[p, 1, rr, :] + pb[p, rr, :]
        add_rows(BLK, 32, 0, both)
        z_send(p).start()

        def keep(rr, i):
            rc[p, 1, rr, :] = rc[p, 1, rr, :] + dy[rr, :].astype(F32)
        add_rows(128, 32, tp * 128, keep)

    outs = (y_out, dx_out)

    def out_rows(p, half):
        return pl.ds(pl.multiple_of(p * BLK + half * 128, 128), 128)

    def fb_at(p, a):
        return fb.at[rows(p * 2 + a, 128)]

    def b_send(p, a):
        return remote(fb_at(p, a), outs[a].at[out_rows(p, tp)], bs.at[p, a], br.at[p, a], zdev)

    def b_local(p, a):
        return pltpu.make_async_copy(fb_at(p, a), outs[a].at[out_rows(p, tp)], fl.at[p, a])

    def finalize(p, a):
        if a == 0:
            for rel in range(4):
                y_zsend(p, rel).wait_recv()
        else:
            z_send(p).wait_recv()

        def body(rr, i):
            kr = pl.ds(pl.multiple_of(tp * 128 + i * 32, 32), 32)
            fr = pl.ds(pl.multiple_of((p * 2 + a) * 128 + i * 32, 32), 32)
            fb[fr, :] = (rc[p, a, kr, :] + rz[p, a, rr, :]).astype(BF16)
        add_rows(128, 32, 0, body)
        b_send(p, a).start()
        b_local(p, a).start()

    for m in (0, 1, 2):
        w_local(m).start()
    for m in (0, 1):
        for c in w_direct(m):
            c.start()
    for p in (0, 1):
        for a in (0, 1):
            t_partner(a, p).start()
    for m in (0, 1):
        w_wait(m, 1)
        w_wait(m, 4)
        for c in w_forward(m):
            c.start()
    for c in w_direct(2):
        c.start()

    for p in (0, 1):
        for a in (0, 1):
            t_partner(a, p).wait_recv()
    first_loads = p_loads(0, 0, xb, 0) + p_loads(1, 0, dyb, 1) + p_loads(0, 1, fb, 2)
    for c in first_loads:
        c.start()
    for c in first_loads:
        c.wait()
    everything = pl.ds(0, 2 * BLK)
    transposes(xb, dyb, everything, 2 * BLK)

    for m in (0, 1):
        w_local(m).wait()
        for slot in (0, 2, 3, 5, 6):
            w_wait(m, slot)

    def silu_up(a, b):
        return (a * jax.nn.sigmoid(a) * b).astype(BF16)

    def early0(cols):
        a = dot(xb[...], wg[:, cols], NN)
        b = dot(xb[...], wu[:, cols], NN)
        pb[0, :, cols], pb[1, :, cols] = a, b
        hb[:, cols] = silu_up(a, b)
    tiles(early0)
    a, b = rest_pair(xb, everything)
    pb[0, :, rest], pb[1, :, rest] = a, b
    hb[:, rest] = silu_up(a, b)
    w_local(2).wait()
    w_wait(2, 0)
    y_group(0, 0)

    def early1(cols):
        a = dot(fb[...], wg[:, cols], NN)
        b = dot(fb[...], wu[:, cols], NN)
        dbb[:, cols] = silu_up(a, b)
    tiles(early1)
    a, b = rest_pair(fb, everything)
    dbb[:, rest] = silu_up(a, b)
    y_finish(0, 0)
    y_group(1, 0)

    w_wait(2, 1)
    w_wait(2, 4)
    for c in w_forward(2):
        c.start()
    for j in range(PIECES):
        for a in (0, 1):
            for k in (0, 1):
                t_own(a, j, k).start()
    y_finish(1, 0)
    w_wait(2, 2)
    y_group(0, 1)
    y_group(1, 1)
    w_wait(2, 3)
    y_finish(0, 1)
    y_group(0, 2)
    y_finish(1, 1)
    y_group(1, 2)
    y_finish(0, 2)
    y_finish(1, 2)
    w_wait(2, 5)
    w_wait(2, 6)
    y_group(0, 3)
    y_group(1, 3)

    def late(cols):
        _, dab[:, cols], dbb[:, cols] = gates(pb[0, :, cols], pb[1, :, cols], grad_tile(dyb, everything, cols))
    y_finish(0, 3)
    tiles(late)
    late(rest)
    y_finish(1, 3)
    for p in (0, 1):
        for rel in range(4):
            y_send(p, rel).wait_send()
    dy1_loads = p_loads(1, 1, xb, 0)
    for c in dy1_loads:
        c.start()
    dx_block(0)
    weight_grads(2 * BLK, first=True)
    dx_finish(0, dyb)
    for c in dy1_loads:
        c.wait()
    transposes(fb, xb, everything, 2 * BLK)
    phase1(fb, xb, everything, everything)
    dx_block(1)
    finalize(0, 0)
    weight_grads(2 * BLK)
    dx_finish(1, xb)
    finalize(1, 0)

    def unit_of(k):
        late_unit = k // (2 * PIECES)
        return ((1 - late_unit) * (1 + lax.rem(k, 2)) + late_unit * 3,
                (1 - late_unit) * (k // 2) + late_unit * (k - 2 * PIECES))

    def service(k):
        rel, j = unit_of(k)
        slot = lax.rem(k, 2)
        for a in (0, 1):
            t_wait_own(a, rel, j)
            t_share(a, rel, j).start()
            u_load(a, rel, j, 0, slot).start()

        @pl.when(rel == 1 + core)
        def _():
            for a in (0, 1):
                t_forward(a, j).start()

    def other_half(k):
        rel, j = unit_of(k)
        slot = lax.rem(k, 2)
        for a in (0, 1):
            t_share(a, rel, j).wait_recv()
            u_load(a, rel, j, 1, slot).start()

    service(jnp.int32(0))
    other_half(jnp.int32(0))

    def unit(k, carry):
        rel, j = unit_of(k)
        slot = lax.rem(k, 2)
        ahead = k < 2 * PIECES

        @pl.when(ahead)
        def _():
            service(k + 1)

        for half in (0, 1):
            for a in (0, 1):
                u_load(a, rel, j, half, slot).wait()
        r = pl.ds(pl.multiple_of(slot * BLK, BLK), BLK)
        phase1(xb, dyb, r, pl.ds(0, BLK))
        transposes(xb, dyb, r, BLK)

        @pl.when(ahead)
        def _():
            other_half(k + 1)
        weight_grads(BLK)

        @pl.when(jnp.logical_and(k >= 2 * PIECES, k < 3 * PIECES - 1))
        def _():
            service(k + 1)
            other_half(k + 1)

        for p in (0, 1):
            @pl.when(k == 2 + 3 * p)
            def _():
                finalize(p, 1)
        return carry
    lax.fori_loop(0, 3 * PIECES, unit, 0)

    grads = (dwg_out, dwu_out, dwd_out)

    def g_part(n, c):
        return acc.at[n, pl.ds(pl.multiple_of(c * ROWS, ROWS), ROWS), :]

    def g_at(n):
        return grads[n].at[:, pl.ds(pl.multiple_of(core * FQ, 128), FQ)]

    g_send = [remote(g_part(n, 1 - core), g_at(n), ds.at[n], dr.at[n], partner) for n in range(3)]
    g_local = [pltpu.make_async_copy(g_part(n, core), g_at(n), dl.at[n]) for n in range(3)]
    for n in range(3):
        g_send[n].start()
        g_local[n].start()

    for m in (0, 1, 2):
        for c in w_direct(m) + w_forward(m):
            c.wait_send()
    for a in (0, 1):
        for j in range(PIECES):
            for k in (0, 1):
                t_own(a, j, k).wait_send()
            t_forward(a, j).wait_send()
            for rel in (1, 2, 3):
                t_share(a, rel, j).wait_send()
    for p in (0, 1):
        for rel in range(4):
            y_zsend(p, rel).wait_send()
        c_send(p).wait_send()
        z_send(p).wait_send()
        for a in (0, 1):
            t_partner(a, p).wait_send()
            b_local(p, a).wait()
            b_send(p, a).wait()
    for n in range(3):
        g_local[n].wait()
        g_send[n].wait()


def write_out(y, dx, g, u, d, y_o, dx_o, g_o, u_o, d_o, yv, dxv, gv, uv, dv, tv, rs, ss):
    loads = [pltpu.make_async_copy(src, dst, rs.at[i])
             for i, (src, dst) in enumerate(((d, dv), (y, yv), (dx, dxv), (g, gv), (u, uv)))]
    stores = [pltpu.make_async_copy(src, dst, ss.at[i])
              for i, (src, dst) in enumerate(((tv, d_o), (yv, y_o), (dxv, dx_o), (gv, g_o), (uv, u_o)))]
    for c in loads:
        c.start()
    loads[0].wait()

    def step(i, carry):
        tv[pl.ds(pl.multiple_of(i * 256, 256), 256), :] = dv[:, pl.ds(pl.multiple_of(i * 256, 256), 256)].T
        return carry
    for i in (1, 2):
        loads[i].wait()
        stores[i].start()
    lax.fori_loop(0, FH // 256, step, 0)
    stores[0].start()
    for i in (3, 4):
        loads[i].wait()
        stores[i].start()
    for c in stores:
        c.wait()


def solution(mesh):
    sds = jax.ShapeDtypeStruct
    dma, vmem = pltpu.SemaphoreType.DMA, pltpu.VMEM

    def device_pass(x, wg, wu, wd, dy):
        anyspec = pl.BlockSpec(memory_space=pl.ANY)
        out = pl.pallas_call(
            kernel,
            out_shape=[sds((TOK, D), BF16), sds((TOK, D), BF16), sds((ROWS, FH), F32), sds((ROWS, FH), F32),
                       sds((ROWS, FH), F32), sds((8, TOK, D), BF16), sds((8, TOK, D), BF16)],
            in_specs=[anyspec] * 5,
            out_specs=[anyspec] * 7,
            scratch_shapes=[
                vmem((D, FQ), BF16), vmem((D, FQ), BF16), vmem((8, FQ, ROWS), BF16),
                vmem((3, 512, FQ), F32),
                vmem((2 * BLK, D), BF16), vmem((2 * BLK, D), BF16),
                vmem((2 * BLK, FQ), BF16), vmem((2 * BLK, FQ), BF16), vmem((2 * BLK, FQ), BF16),
                vmem((2, 2 * BLK, D), F32), vmem((2, 2, BLK, D), F32), vmem((2, 2, 128, D), F32),
                vmem((2 * BLK, D), BF16),
                vmem((512, 2 * BLK), BF16), vmem((512, 2 * BLK), BF16),
                dma((3,)), dma((3, 7)), dma((3, 7)),
                dma((8, 2)), dma((2, 2)), dma((2, 2)),
                dma((PIECES, 2, 2)), dma((PIECES, 2)), dma((4, PIECES, 2)), dma((4, PIECES, 2)), dma((4, PIECES, 2)),
                dma((2, 4)), dma((2, 4)), dma((2, 4)), dma((2, 4)),
                dma((2,)), dma((2,)), dma((2,)), dma((2,)), dma((2, 2)), dma((2, 2)), dma((2, 2)),
                dma((3,)), dma((3,)), dma((3,)),
            ],
            compiler_params=pltpu.CompilerParams(collective_id=0, has_side_effects=True,
                                                 vmem_limit_bytes=67043328),
        )(x, wg, wu, wd, dy)
        shapes = [((TOK, D), BF16)] * 2 + [((ROWS, FH), F32)] * 3
        return pl.pallas_call(
            write_out,
            out_shape=[sds(*s) for s in shapes[:4]] + [sds((FH, ROWS), F32)],
            in_specs=[anyspec] * 5,
            out_specs=[anyspec] * 5,
            scratch_shapes=[vmem(*s) for s in shapes] + [vmem((FH, ROWS), F32), dma((5,)), dma((5,))],
            compiler_params=pltpu.CompilerParams(vmem_limit_bytes=67043328),
        )(*out[:5])

    row_spec = P('dp', None)
    weight_spec = P('dp', 'tp')
    down_spec = P('tp', 'dp')
    return jax.shard_map(device_pass, mesh=mesh,
                         in_specs=(row_spec, weight_spec, weight_spec, down_spec, row_spec),
                         out_specs=(row_spec, row_spec, weight_spec, weight_spec, down_spec),
                         check_vma=False)
```

```python
import functools

import jax
import jax.numpy as jnp
from jax import lax
from jax.experimental import pallas as pl
from jax.experimental.pallas import tpu as pltpu
from jax.sharding import PartitionSpec as P

MESH = pl.DeviceIdType.MESH
BOTH = (0, 1)
BF16, F32 = jnp.bfloat16, jnp.float32
D, FH, FQ, ROWS, TOK = 2048, 2816, 1408, 256, 512
SUB, BLK, PIECES = 128, 256, 4
NN = (((1,), (0,)), ((), ()))
NT = (((1,), (1,)), ((), ()))


def dot(a, b, dims):
    return lax.dot_general(a, b, dims, preferred_element_type=F32)


def kernel(x_in, wg_in, wu_in, wd_in, dy_in,
           y_out, dx_out, dwg_out, dwu_out, dwd_out, x_all, dy_all,
           wg, wu, wd, acc, xb, dyb, hb, dab, dbb, pb, rc, rz, fb, xt, dyt, ab,
           wl, ws, wr, xl, os, orr, es, er, ezs, ezr, xs, xf, xd, xr, pr, ys, yr, vs, vr, cs, cr, zs, zr, bs, br, fl, ds, dr, dl):
    tp, dp = lax.axis_index('tp'), lax.axis_index('dp')
    core, xc, yc = lax.rem(dp, 2), lax.rem(lax.div(dp, 2), 2), lax.div(dp, 4)
    col = lax.div(dp, 2)

    def idx(yy, xx, cc):
        return yy * 4 + xx * 2 + cc

    def dev(yy, xx, cc):
        return (tp, idx(yy, xx, cc))

    partner = dev(yc, xc, 1 - core)
    zdev = (1 - tp, dp)

    barrier = pltpu.get_barrier_semaphore()
    peers = [partner, zdev] + [dev(yc, 1 - xc, cc) for cc in BOTH] + [dev(1 - yc, xc, cc) for cc in BOTH]
    for peer in peers:
        pl.semaphore_signal(barrier, inc=1, device_id=peer, device_id_type=MESH)
    pl.semaphore_wait(barrier, len(peers))

    def remote(src, dst, ssem, rsem, device):
        return pltpu.make_async_remote_copy(src_ref=src, dst_ref=dst, send_sem=ssem, recv_sem=rsem,
                                            device_id=device, device_id_type=MESH)

    def w_src(m, cc):
        if m == 2:
            return wd_in.at[pl.ds(pl.multiple_of(cc * FQ, 128), FQ), :]
        return (wg_in, wu_in)[m].at[:, pl.ds(pl.multiple_of(cc * FQ, 128), FQ)]

    def w_at(m, r):
        if m == 2:
            return wd.at[r]
        return (wg, wu)[m].at[pl.ds(pl.multiple_of(r * ROWS, ROWS), ROWS), :]

    def w_local(m):
        return pltpu.make_async_copy(w_src(m, core), w_at(m, dp), wl.at[m])

    def w_direct(m):
        out = [remote(w_src(m, 1 - core), w_at(m, dp), ws.at[m, 0], wr.at[m, 0], partner)]
        for cc in BOTH:
            out.append(remote(w_src(m, cc), w_at(m, dp), ws.at[m, 1 + cc], wr.at[m, 1 + core], dev(yc, 1 - xc, cc)))
            out.append(remote(w_src(m, cc), w_at(m, dp), ws.at[m, 3 + cc], wr.at[m, 3 + core], dev(1 - yc, xc, cc)))
        return out

    rx, ry = idx(yc, 1 - xc, 0), idx(1 - yc, xc, 1)

    def w_forward(m):
        return [remote(w_at(m, rx), w_at(m, rx), ws.at[m, 5], wr.at[m, 5], dev(1 - yc, xc, core)),
                remote(w_at(m, ry), w_at(m, ry), ws.at[m, 6], wr.at[m, 6], dev(yc, 1 - xc, core))]

    def w_wait(m, slot):
        remote(w_at(m, dp), w_at(m, dp), ws.at[m, slot], wr.at[m, slot], partner).wait_recv()

    arrays = ((x_in, x_all), (dy_in, dy_all))

    def rows(j, size=SUB):
        return pl.ds(pl.multiple_of(j * size, size), size)

    def t_at(a, rel, s, j):
        return arrays[a][1].at[rel * 2 + s, rows(j)]

    def t_partner(a, p):
        return remote(arrays[a][0].at[rows(p, BLK)], arrays[a][1].at[core, rows(p, BLK)],
                      os.at[p, a], orr.at[p, a], partner)

    def t_own(a, j, k):
        return remote(arrays[a][0].at[rows(j)], t_at(a, 1 + k, core, j), xs.at[j, a, k], xr.at[1 + k, j, a],
                      (dev(yc, 1 - xc, core), dev(1 - yc, xc, core))[k])

    def t_share(a, rel, j):
        return remote(t_at(a, rel, core, j), t_at(a, rel, core, j), xd.at[rel, j, a], pr.at[rel, j, a], partner)

    fwd_dev = dev(yc + (1 - core) * (1 - 2 * yc), xc + core * (1 - 2 * xc), core)

    def t_forward(a, j):
        return remote(t_at(a, 1 + core, core, j), t_at(a, 3, core, j), xf.at[j, a], xr.at[3, j, a], fwd_dev)

    def t_wait_own(a, rel, j):
        remote(t_at(a, rel, core, j), t_at(a, rel, core, j), xd.at[rel, j, a], xr.at[rel, j, a], partner).wait_recv()

    def p_loads(a, p, ref, sem):
        return [pltpu.make_async_copy(arrays[a][0].at[rows(p, BLK)], ref.at[pl.ds(0, BLK)], xl.at[sem, 0]),
                pltpu.make_async_copy(arrays[a][1].at[1 - core, rows(p, BLK)], ref.at[pl.ds(BLK, BLK)], xl.at[sem, 1])]

    bufs = (xb, dyb)

    def u_load(a, rel, j, half, slot):
        source = core if half == 0 else 1 - core
        return pltpu.make_async_copy(t_at(a, rel, source, j),
                                     bufs[a].at[pl.ds(pl.multiple_of(slot * BLK + half * SUB, SUB), SUB)],
                                     xl.at[4 + slot * 2 + half, a])

    def e_own(a, k):
        return remote(arrays[a][0].at[rows(0)], t_at(a, 1 + k, core, 0), es.at[k], er.at[1 + k],
                      (dev(yc, 1 - xc, core), dev(1 - yc, xc, core))[k])

    def e_zshare(a, rel):
        return remote(t_at(a, rel, core, 0), t_at(a, rel, core, 0), ezs.at[rel], ezr.at[rel], zdev)

    def on_plane(body):
        for a in BOTH:
            @pl.when(tp == a)
            def _(a=a):
                body(a)

    def e_arrived(rel):
        def body(a):
            remote(t_at(a, rel, core, 0), t_at(a, rel, core, 0), ezs.at[rel], er.at[rel], partner).wait_recv()
            e_zshare(a, rel).start()
            t_share(a, rel, 0).start()
        on_plane(body)

    def e_crossed(rel):
        def body(a):
            e_zshare(1 - a, rel).wait_recv()
            t_share(1 - a, rel, 0).start()
        on_plane(body)

    def gates(a, b, g):
        s = jax.nn.sigmoid(a)
        silu = a * s
        return ((silu * b).astype(BF16), (g * b * s * (1.0 + a * (1.0 - s))).astype(BF16), (g * silu).astype(BF16))

    main, rest = FQ // 256, pl.ds(FQ // 256 * 256, FQ % 256)

    def tiles(body, unroll=False):
        def step(n, carry):
            body(pl.ds(pl.multiple_of(n * 256, 256), 256))
            return carry
        lax.fori_loop(0, main, step, 0, unroll=unroll)

    def grad_tile(dy, r, cols):
        g = dot(dy[r, 0:ROWS], wd[0, cols, :], NT)
        for i in range(1, 8):
            g = g + dot(dy[r, i * ROWS:(i + 1) * ROWS], wd[i, cols, :], NT)
        return g

    def rest_pair(x, r):
        both = dot(x[r, :], jnp.concatenate([wg[:, rest], wu[:, rest]], axis=1), NN)
        return both[:, 0:FQ % 256], both[:, FQ % 256:]

    def phase1(x, dy, r, o, unroll=False):
        def body(cols):
            a = dot(x[r, :], wg[:, cols], NN)
            b = dot(x[r, :], wu[:, cols], NN)
            hb[o, cols], dab[o, cols], dbb[o, cols] = gates(a, b, grad_tile(dy, r, cols))
        tiles(body, unroll)
        a, b = rest_pair(x, r)
        hb[o, rest], dab[o, rest], dbb[o, rest] = gates(a, b, grad_tile(dy, r, rest))

    def transposes(x, dy, r, size):
        own_cols = pl.ds(pl.multiple_of(col * 512, 512), 512)
        xt[:, 0:size] = x[r, own_cols].T
        dyt[:, 0:size] = dy[r, own_cols].T

    def weight_grads(size, first=False, unroll=False):
        o = pl.ds(0, size)

        def put(n, cols, value):
            acc[n, :, cols] = value if first else acc[n, :, cols] + value

        def body(cols):
            put(0, cols, dot(xt[:, 0:size], dab[o, cols], NN))
            put(1, cols, dot(xt[:, 0:size], dbb[o, cols], NN))
            put(2, cols, dot(dyt[:, 0:size], hb[o, cols], NN))
        tiles(body, unroll)
        both = dot(xt[:, 0:size], jnp.concatenate([dab[o, rest], dbb[o, rest]], axis=1), NN)
        put(0, rest, both[:, 0:FQ % 256])
        put(1, rest, both[:, FQ % 256:])
        put(2, rest, dot(dyt[:, 0:size], hb[o, rest], NN))

    cols_of = [pl.ds(pl.multiple_of(q * 512, 512), 512)
               for q in (col, yc * 2 + 1 - xc, (1 - yc) * 2 + xc, (1 - yc) * 2 + 1 - xc)]
    first_of = [q * 2 for q in (col, yc * 2 + 1 - xc, (1 - yc) * 2 + xc, (1 - yc) * 2 + 1 - xc)]

    def y_buf(p, rel):
        k = p * 4 + rel
        return (acc, k // 2, k % 2 * 512) if k < 6 else (pb, k - 6, FQ)

    def y_send(p, rel):
        ref, n, off = y_buf(p, rel)
        return remote(ref.at[n, pl.ds(BLK, BLK), pl.ds(off, 512)], rc.at[p, 0, :, cols_of[rel]],
                      ys.at[p, rel], yr.at[p, rel], partner)

    def y_zsend(p, rel):
        return remote(rc.at[p, 0, rows(1 - tp, 128), cols_of[rel]], rz.at[p, 0, :, cols_of[rel]],
                      vs.at[p, rel], vr.at[p, rel], zdev)

    def y_group(p, rel):
        ref, n, off = y_buf(p, rel)
        h = (hb, dbb)[p]

        def step(i, carry):
            ref[n, :, pl.ds(pl.multiple_of(off + i * ROWS, 128), ROWS)] = dot(h[...], wd[first_of[rel] + i], NN)
            return carry
        lax.fori_loop(0, 2, step, 0)
        y_send(p, rel).start()

    def add_rows(total, count, base, body):
        def step(i, carry):
            body(pl.ds(pl.multiple_of(base + i * count, count), count), i)
            return carry
        lax.fori_loop(0, total // count, step, 0)

    def y_finish(p, rel):
        ref, n, off = y_buf(p, rel)
        cols = cols_of[rel]
        y_send(p, rel).wait_recv()

        def both(rr, i):
            rc[p, 0, rr, cols] = rc[p, 0, rr, cols] + ref[n, rr, pl.ds(off, 512)]
        add_rows(BLK, 64, 0, both)
        y_zsend(p, rel).start()
        x = (xb, fb)[p]

        def keep(rr, i):
            rc[p, 0, rr, cols] = rc[p, 0, rr, cols] + x[rr, cols].astype(F32)
        add_rows(128, 64, tp * 128, keep)

    def dx_block(p):
        def step(i, carry):
            cols = pl.ds(pl.multiple_of(i * ROWS, ROWS), ROWS)
            pb[p, :, cols] = dot(dab[...], wg[cols, :], NT) + dot(dbb[...], wu[cols, :], NT)
            return carry
        lax.fori_loop(0, 8, step, 0, unroll=2)
        c_send(p).start()

    def c_send(p):
        return remote(pb.at[p, pl.ds(BLK, BLK)], rc.at[p, 1], cs.at[p], cr.at[p], partner)

    def z_send(p):
        return remote(rc.at[p, 1, rows(1 - tp, 128)], rz.at[p, 1], zs.at[p], zr.at[p], zdev)

    def dx_finish(p, dy):
        c_send(p).wait_recv()

        def both(rr, i):
            rc[p, 1, rr, :] = rc[p, 1, rr, :] + pb[p, rr, :]
        add_rows(BLK, 32, 0, both)
        z_send(p).start()

        def keep(rr, i):
            rc[p, 1, rr, :] = rc[p, 1, rr, :] + dy[rr, :].astype(F32)
        add_rows(128, 32, tp * 128, keep)

    outs = (y_out, dx_out)

    def out_rows(p, half):
        return pl.ds(pl.multiple_of(p * BLK + half * 128, 128), 128)

    def fb_at(p, a):
        return fb.at[rows(p * 2 + a, 128)]

    def b_send(p, a):
        return remote(fb_at(p, a), outs[a].at[out_rows(p, tp)], bs.at[p, a], br.at[p, a], zdev)

    def b_local(p, a):
        return pltpu.make_async_copy(fb_at(p, a), outs[a].at[out_rows(p, tp)], fl.at[p, a])

    def finalize(p, a):
        if a == 0:
            for rel in range(4):
                y_zsend(p, rel).wait_recv()
        else:
            z_send(p).wait_recv()

        def body(rr, i):
            kr = pl.ds(pl.multiple_of(tp * 128 + i * 32, 32), 32)
            fr = pl.ds(pl.multiple_of((p * 2 + a) * 128 + i * 32, 32), 32)
            fb[fr, :] = (rc[p, a, kr, :] + rz[p, a, rr, :]).astype(BF16)
        add_rows(128, 32, 0, body)
        b_send(p, a).start()
        b_local(p, a).start()

    on_plane(lambda a: [e_own(a, k).start() for k in BOTH])
    for m in BOTH:
        for c in w_direct(m):
            c.start()
    for m in (0, 1, 2):
        w_local(m).start()
    for p in BOTH:
        for a in BOTH:
            t_partner(a, p).start()
    e_arrived(1)
    e_arrived(2)
    e_crossed(1)
    e_crossed(2)
    for m in BOTH:
        w_wait(m, 1)
        w_wait(m, 4)
        for c in w_forward(m):
            c.start()
    for c in w_direct(2):
        c.start()

    for p in BOTH:
        for a in BOTH:
            t_partner(a, p).wait_recv()
    first_loads = p_loads(0, 0, xb, 0) + p_loads(1, 0, dyb, 1) + p_loads(0, 1, fb, 2)
    for c in first_loads:
        c.start()
    for c in first_loads:
        c.wait()
    everything = pl.ds(0, 2 * BLK)
    transposes(xb, dyb, everything, 2 * BLK)

    for m in BOTH:
        w_local(m).wait()
        for slot in (0, 2, 3, 5, 6):
            w_wait(m, slot)

    def silu_up(a, b):
        return (a * jax.nn.sigmoid(a) * b).astype(BF16)

    def early0(cols):
        a = dot(xb[...], wg[:, cols], NN)
        b = dot(xb[...], wu[:, cols], NN)
        pb[0, :, cols], pb[1, :, cols] = a, b
        hb[:, cols] = silu_up(a, b)
    tiles(early0)
    a, b = rest_pair(xb, everything)
    pb[0, :, rest], pb[1, :, rest] = a, b
    hb[:, rest] = silu_up(a, b)
    w_local(2).wait()
    w_wait(2, 0)
    y_group(0, 0)

    def early1(cols):
        a = dot(fb[...], wg[:, cols], NN)
        b = dot(fb[...], wu[:, cols], NN)
        ab[0, :, cols], ab[1, :, cols] = a, b
        dbb[:, cols] = silu_up(a, b)
    tiles(early1)
    a, b = rest_pair(fb, everything)
    ab[0, :, rest], ab[1, :, rest] = a, b
    dbb[:, rest] = silu_up(a, b)
    y_finish(0, 0)
    y_group(1, 0)

    w_wait(2, 1)
    w_wait(2, 4)
    for c in w_forward(2):
        c.start()
    for j in range(1, PIECES):
        for a in BOTH:
            for k in BOTH:
                t_own(a, j, k).start()
    for a in BOTH:
        t_forward(a, 0).start()
    y_finish(1, 0)
    w_wait(2, 2)
    y_group(0, 1)
    y_group(1, 1)
    w_wait(2, 3)
    y_finish(0, 1)
    y_group(0, 2)
    y_finish(1, 1)
    y_group(1, 2)
    y_finish(0, 2)
    y_finish(1, 2)
    w_wait(2, 5)
    w_wait(2, 6)
    y_group(0, 3)
    y_group(1, 3)

    def late(cols):
        _, dab[:, cols], dbb[:, cols] = gates(pb[0, :, cols], pb[1, :, cols], grad_tile(dyb, everything, cols))
    y_finish(0, 3)
    tiles(late)
    late(rest)
    y_finish(1, 3)
    for p in BOTH:
        for rel in range(4):
            y_send(p, rel).wait_send()
    dy1_loads = p_loads(1, 1, xb, 0)
    for c in dy1_loads:
        c.start()
    dx_block(0)
    weight_grads(2 * BLK, first=True)
    dx_finish(0, dyb)
    for c in dy1_loads:
        c.wait()
    transposes(fb, xb, everything, 2 * BLK)

    def late1(cols):
        g = grad_tile(xb, everything, cols)
        hb[:, cols], dab[:, cols], dbb[:, cols] = gates(ab[0, :, cols], ab[1, :, cols], g)
    tiles(late1)
    late1(rest)
    dx_block(1)
    finalize(0, 0)
    weight_grads(2 * BLK)
    dx_finish(1, xb)
    finalize(1, 0)

    def unit_of(k):
        diag = k // (2 * PIECES)
        return ((1 - diag) * (1 + lax.rem(k, 2)) + diag * 3,
                (1 - diag) * (k // 2) + diag * (k - 2 * PIECES))

    def service(k):
        rel, j = unit_of(k)
        slot = lax.rem(k, 2)
        for a in BOTH:
            @pl.when(k > 1)
            def _(a=a):
                t_wait_own(a, rel, j)
                t_share(a, rel, j).start()
            u_load(a, rel, j, 0, slot).start()

        @pl.when(jnp.logical_and(k > 1, rel == 1 + core))
        def _():
            for a in BOTH:
                t_forward(a, j).start()

    def other_half(k):
        rel, j = unit_of(k)
        slot = lax.rem(k, 2)
        for a in BOTH:
            t_share(a, rel, j).wait_recv()
            u_load(a, rel, j, 1, slot).start()

    service(jnp.int32(0))
    other_half(jnp.int32(0))
    last = 3 * PIECES - 1

    def unit(k, carry):
        rel, j = unit_of(k)
        slot = lax.rem(k, 2)

        @pl.when(k < last - 0)
        def _():
            service(k + 1)

        for half in BOTH:
            for a in BOTH:
                u_load(a, rel, j, half, slot).wait()
        r = pl.ds(pl.multiple_of(slot * BLK, BLK), BLK)
        phase1(xb, dyb, r, pl.ds(0, BLK), True)
        transposes(xb, dyb, r, BLK)

        @pl.when(k < last - 0)
        def _():
            other_half(k + 1)
        weight_grads(BLK, unroll=True)

        @pl.when(jnp.logical_and(k >= last - 0, k < last))
        def _():
            service(k + 1)
            other_half(k + 1)

        for p in BOTH:
            @pl.when(k == 4 + 3 * p)
            def _():
                finalize(p, 1)
        return carry
    lax.fori_loop(0, 3 * PIECES, unit, 0)

    grads = (dwg_out, dwu_out, dwd_out)

    def g_part(n, c):
        return acc.at[n, pl.ds(pl.multiple_of(c * ROWS, ROWS), ROWS), :]

    def g_at(n):
        return grads[n].at[:, pl.ds(pl.multiple_of(core * FQ, 128), FQ)]

    g_send = [remote(g_part(n, 1 - core), g_at(n), ds.at[n], dr.at[n], partner) for n in range(3)]
    g_local = [pltpu.make_async_copy(g_part(n, core), g_at(n), dl.at[n]) for n in range(3)]
    for n in range(3):
        g_send[n].start()
        g_local[n].start()

    for m in (0, 1, 2):
        for c in w_direct(m) + w_forward(m):
            c.wait_send()
    for a in BOTH:
        for j in range(PIECES):
            if j:
                for k in BOTH:
                    t_own(a, j, k).wait_send()
            t_forward(a, j).wait_send()
            for rel in (1, 2, 3):
                t_share(a, rel, j).wait_send()

    def e_drain(a):
        for k in BOTH:
            e_own(a, k).wait_send()
        for rel in (1, 2):
            e_zshare(a, rel).wait_send()
    on_plane(e_drain)
    for p in BOTH:
        for rel in range(4):
            y_zsend(p, rel).wait_send()
        c_send(p).wait_send()
        z_send(p).wait_send()
        for a in BOTH:
            t_partner(a, p).wait_send()
            b_local(p, a).wait()
            b_send(p, a).wait()
    for n in range(3):
        g_local[n].wait()
        g_send[n].wait()


def write_out(y, dx, g, u, d, y_o, dx_o, g_o, u_o, d_o, yv, dxv, gv, uv, dv, tv, rs, ss):
    loads = [pltpu.make_async_copy(src, dst, rs.at[i])
             for i, (src, dst) in enumerate(((d, dv), (y, yv), (dx, dxv), (g, gv), (u, uv)))]
    stores = [pltpu.make_async_copy(src, dst, ss.at[i])
              for i, (src, dst) in enumerate(((tv, d_o), (yv, y_o), (dxv, dx_o), (gv, g_o), (uv, u_o)))]
    for c in loads:
        c.start()
    loads[0].wait()

    def step(i, carry):
        tv[pl.ds(pl.multiple_of(i * 256, 256), 256), :] = dv[:, pl.ds(pl.multiple_of(i * 256, 256), 256)].T
        return carry
    for i in (1, 2):
        loads[i].wait()
        stores[i].start()
    lax.fori_loop(0, FH // 256, step, 0)
    stores[0].start()
    for i in (3, 4):
        loads[i].wait()
        stores[i].start()
    for c in stores:
        c.wait()


def solution(mesh):
    sds = jax.ShapeDtypeStruct
    dma, vmem = pltpu.SemaphoreType.DMA, pltpu.VMEM

    def device_pass(x, wg, wu, wd, dy):
        anyspec = pl.BlockSpec(memory_space=pl.ANY)
        out = pl.pallas_call(
            kernel,
            out_shape=[sds((TOK, D), BF16), sds((TOK, D), BF16), sds((ROWS, FH), F32), sds((ROWS, FH), F32),
                       sds((ROWS, FH), F32), sds((8, TOK, D), BF16), sds((8, TOK, D), BF16)],
            in_specs=[anyspec] * 5,
            out_specs=[anyspec] * 7,
            scratch_shapes=[
                vmem((D, FQ), BF16), vmem((D, FQ), BF16), vmem((8, FQ, ROWS), BF16),
                vmem((3, 512, FQ), F32),
                vmem((2 * BLK, D), BF16), vmem((2 * BLK, D), BF16),
                vmem((2 * BLK, FQ), BF16), vmem((2 * BLK, FQ), BF16), vmem((2 * BLK, FQ), BF16),
                vmem((2, 2 * BLK, D), F32), vmem((2, 2, BLK, D), F32), vmem((2, 2, 128, D), F32),
                vmem((2 * BLK, D), BF16),
                vmem((512, 2 * BLK), BF16), vmem((512, 2 * BLK), BF16),
                vmem((2, 2 * BLK, FQ), F32),
                dma((3,)), dma((3, 7)), dma((3, 7)),
                dma((8, 2)), dma((2, 2)), dma((2, 2)),
                dma((2,)), dma((3,)), dma((3,)), dma((3,)),
                dma((PIECES, 2, 2)), dma((PIECES, 2)), dma((4, PIECES, 2)), dma((4, PIECES, 2)), dma((4, PIECES, 2)),
                dma((2, 4)), dma((2, 4)), dma((2, 4)), dma((2, 4)),
                dma((2,)), dma((2,)), dma((2,)), dma((2,)), dma((2, 2)), dma((2, 2)), dma((2, 2)),
                dma((3,)), dma((3,)), dma((3,)),
            ],
            compiler_params=pltpu.CompilerParams(collective_id=0, has_side_effects=True,
                                                 vmem_limit_bytes=67043328),
        )(x, wg, wu, wd, dy)
        shapes = [((TOK, D), BF16)] * 2 + [((ROWS, FH), F32)] * 3
        return pl.pallas_call(
            write_out,
            out_shape=[sds(*s) for s in shapes[:4]] + [sds((FH, ROWS), F32)],
            in_specs=[anyspec] * 5,
            out_specs=[anyspec] * 5,
            scratch_shapes=[vmem(*s) for s in shapes] + [vmem((FH, ROWS), F32), dma((5,)), dma((5,))],
            compiler_params=pltpu.CompilerParams(vmem_limit_bytes=67043328),
        )(*out[:5])

    row_spec = P('dp', None)
    weight_spec = P('dp', 'tp')
    down_spec = P('tp', 'dp')
    return jax.shard_map(device_pass, mesh=mesh,
                         in_specs=(row_spec, weight_spec, weight_spec, down_spec, row_spec),
                         out_specs=(row_spec, row_spec, weight_spec, weight_spec, down_spec),
                         check_vma=False)
```

```python
import functools

import jax
import jax.numpy as jnp
from jax import lax
from jax.experimental import pallas as pl
from jax.experimental.pallas import tpu as pltpu
from jax.sharding import PartitionSpec as P

MESH = pl.DeviceIdType.MESH
BOTH = (0, 1)
BF16, F32 = jnp.bfloat16, jnp.float32
D, FH, FQ, ROWS, TOK = 2048, 2816, 1408, 256, 512
SUB, BLK, PIECES = 128, 256, 4
NN = (((1,), (0,)), ((), ()))
NT = (((1,), (1,)), ((), ()))


def dot(a, b, dims):
    return lax.dot_general(a, b, dims, preferred_element_type=F32)


def kernel(x_in, wg_in, wu_in, wd_in, dy_in,
           y_out, dx_out, dwg_out, dwu_out, dwd_out, x_all, dy_all,
           wg, wu, wd, acc, xb, dyb, hb, dab, dbb, pb, rc, rz, fb, xt, dyt, ab,
           wl, ws, wr, xl, os, orr, es, er, ezs, ezr, xs, xf, xd, xr, pr, ys, yr, vs, vr, cs, cr, zs, zr, bs, br, fl, ds, dr, dl):
    tp, dp = lax.axis_index('tp'), lax.axis_index('dp')
    core, xc, yc = lax.rem(dp, 2), lax.rem(lax.div(dp, 2), 2), lax.div(dp, 4)
    col = lax.div(dp, 2)

    def idx(yy, xx, cc):
        return yy * 4 + xx * 2 + cc

    def dev(yy, xx, cc):
        return (tp, idx(yy, xx, cc))

    partner = dev(yc, xc, 1 - core)
    zdev = (1 - tp, dp)

    barrier = pltpu.get_barrier_semaphore()
    peers = [partner, zdev] + [dev(yc, 1 - xc, cc) for cc in BOTH] + [dev(1 - yc, xc, cc) for cc in BOTH]
    for peer in peers:
        pl.semaphore_signal(barrier, inc=1, device_id=peer, device_id_type=MESH)
    pl.semaphore_wait(barrier, len(peers))

    def remote(src, dst, ssem, rsem, device):
        return pltpu.make_async_remote_copy(src_ref=src, dst_ref=dst, send_sem=ssem, recv_sem=rsem,
                                            device_id=device, device_id_type=MESH)

    def w_src(m, cc):
        if m == 2:
            return wd_in.at[pl.ds(pl.multiple_of(cc * FQ, 128), FQ), :]
        return (wg_in, wu_in)[m].at[:, pl.ds(pl.multiple_of(cc * FQ, 128), FQ)]

    def w_at(m, r):
        if m == 2:
            return wd.at[r]
        return (wg, wu)[m].at[pl.ds(pl.multiple_of(r * ROWS, ROWS), ROWS), :]

    def w_local(m):
        return pltpu.make_async_copy(w_src(m, core), w_at(m, dp), wl.at[m])

    def w_direct(m):
        out = [remote(w_src(m, 1 - core), w_at(m, dp), ws.at[m, 0], wr.at[m, 0], partner)]
        for cc in BOTH:
            out.append(remote(w_src(m, cc), w_at(m, dp), ws.at[m, 1 + cc], wr.at[m, 1 + core], dev(yc, 1 - xc, cc)))
            out.append(remote(w_src(m, cc), w_at(m, dp), ws.at[m, 3 + cc], wr.at[m, 3 + core], dev(1 - yc, xc, cc)))
        return out

    rx, ry = idx(yc, 1 - xc, 0), idx(1 - yc, xc, 1)

    def w_forward(m):
        return [remote(w_at(m, rx), w_at(m, rx), ws.at[m, 5], wr.at[m, 5], dev(1 - yc, xc, core)),
                remote(w_at(m, ry), w_at(m, ry), ws.at[m, 6], wr.at[m, 6], dev(yc, 1 - xc, core))]

    def w_wait(m, slot):
        remote(w_at(m, dp), w_at(m, dp), ws.at[m, slot], wr.at[m, slot], partner).wait_recv()

    arrays = ((x_in, x_all), (dy_in, dy_all))

    def rows(j, size=SUB):
        return pl.ds(pl.multiple_of(j * size, size), size)

    def t_at(a, rel, s, j):
        return arrays[a][1].at[rel * 2 + s, rows(j)]

    def t_partner(a, p):
        return remote(arrays[a][0].at[rows(p, BLK)], arrays[a][1].at[core, rows(p, BLK)],
                      os.at[p, a], orr.at[p, a], partner)

    def t_own(a, j, k):
        return remote(arrays[a][0].at[rows(j)], t_at(a, 1 + k, core, j), xs.at[j, a, k], xr.at[1 + k, j, a],
                      (dev(yc, 1 - xc, core), dev(1 - yc, xc, core))[k])

    def t_share(a, rel, j):
        return remote(t_at(a, rel, core, j), t_at(a, rel, core, j), xd.at[rel, j, a], pr.at[rel, j, a], partner)

    fwd_dev = dev(yc + (1 - core) * (1 - 2 * yc), xc + core * (1 - 2 * xc), core)

    def t_forward(a, j):
        return remote(t_at(a, 1 + core, core, j), t_at(a, 3, core, j), xf.at[j, a], xr.at[3, j, a], fwd_dev)

    def t_wait_own(a, rel, j):
        remote(t_at(a, rel, core, j), t_at(a, rel, core, j), xd.at[rel, j, a], xr.at[rel, j, a], partner).wait_recv()

    def p_loads(a, p, ref, sem):
        return [pltpu.make_async_copy(arrays[a][0].at[rows(p, BLK)], ref.at[pl.ds(0, BLK)], xl.at[sem, 0]),
                pltpu.make_async_copy(arrays[a][1].at[1 - core, rows(p, BLK)], ref.at[pl.ds(BLK, BLK)], xl.at[sem, 1])]

    bufs = (xb, dyb)

    def u_load(a, rel, j, half, slot):
        source = core if half == 0 else 1 - core
        return pltpu.make_async_copy(t_at(a, rel, source, j),
                                     bufs[a].at[pl.ds(pl.multiple_of(slot * BLK + half * SUB, SUB), SUB)],
                                     xl.at[4 + slot * 2 + half, a])

    def e_own(a, k):
        return remote(arrays[a][0].at[rows(0)], t_at(a, 1 + k, core, 0), es.at[k], er.at[1 + k],
                      (dev(yc, 1 - xc, core), dev(1 - yc, xc, core))[k])

    def e_zshare(a, rel):
        return remote(t_at(a, rel, core, 0), t_at(a, rel, core, 0), ezs.at[rel], ezr.at[rel], zdev)

    def on_plane(body):
        for a in BOTH:
            @pl.when(tp == a)
            def _(a=a):
                body(a)

    def e_arrived(rel):
        def body(a):
            remote(t_at(a, rel, core, 0), t_at(a, rel, core, 0), ezs.at[rel], er.at[rel], partner).wait_recv()
            e_zshare(a, rel).start()
            t_share(a, rel, 0).start()
        on_plane(body)

    def e_crossed(rel):
        def body(a):
            e_zshare(1 - a, rel).wait_recv()
            t_share(1 - a, rel, 0).start()
        on_plane(body)

    def gates(a, b, g):
        s = jax.nn.sigmoid(a)
        silu = a * s
        return ((silu * b).astype(BF16), (g * b * s * (1.0 + a * (1.0 - s))).astype(BF16), (g * silu).astype(BF16))

    main, rest = FQ // 256, pl.ds(FQ // 256 * 256, FQ % 256)

    def tiles(body, unroll=False):
        def step(n, carry):
            body(pl.ds(pl.multiple_of(n * 256, 256), 256))
            return carry
        lax.fori_loop(0, main, step, 0, unroll=unroll)

    def grad_tile(dy, r, cols):
        g = dot(dy[r, 0:ROWS], wd[0, cols, :], NT)
        for i in range(1, 8):
            g = g + dot(dy[r, i * ROWS:(i + 1) * ROWS], wd[i, cols, :], NT)
        return g

    def rest_pair(x, r):
        both = dot(x[r, :], jnp.concatenate([wg[:, rest], wu[:, rest]], axis=1), NN)
        return both[:, 0:FQ % 256], both[:, FQ % 256:]

    def phase1(x, dy, r, o, unroll=False):
        def body(cols):
            a = dot(x[r, :], wg[:, cols], NN)
            b = dot(x[r, :], wu[:, cols], NN)
            hb[o, cols], dab[o, cols], dbb[o, cols] = gates(a, b, grad_tile(dy, r, cols))
        tiles(body, unroll)
        a, b = rest_pair(x, r)
        hb[o, rest], dab[o, rest], dbb[o, rest] = gates(a, b, grad_tile(dy, r, rest))

    def transposes(x, dy, r, size):
        own_cols = pl.ds(pl.multiple_of(col * 512, 512), 512)
        xt[:, 0:size] = x[r, own_cols].T
        dyt[:, 0:size] = dy[r, own_cols].T

    def weight_grads(size, first=False, unroll=False):
        o = pl.ds(0, size)

        def put(n, cols, value):
            acc[n, :, cols] = value if first else acc[n, :, cols] + value

        def body(cols):
            put(0, cols, dot(xt[:, 0:size], dab[o, cols], NN))
            put(1, cols, dot(xt[:, 0:size], dbb[o, cols], NN))
            put(2, cols, dot(dyt[:, 0:size], hb[o, cols], NN))
        tiles(body, unroll)
        both = dot(xt[:, 0:size], jnp.concatenate([dab[o, rest], dbb[o, rest]], axis=1), NN)
        put(0, rest, both[:, 0:FQ % 256])
        put(1, rest, both[:, FQ % 256:])
        put(2, rest, dot(dyt[:, 0:size], hb[o, rest], NN))

    cols_of = [pl.ds(pl.multiple_of(q * 512, 512), 512)
               for q in (col, yc * 2 + 1 - xc, (1 - yc) * 2 + xc, (1 - yc) * 2 + 1 - xc)]
    first_of = [q * 2 for q in (col, yc * 2 + 1 - xc, (1 - yc) * 2 + xc, (1 - yc) * 2 + 1 - xc)]

    def y_buf(p, rel):
        k = p * 4 + rel
        return (acc, k // 2, k % 2 * 512) if k < 6 else (pb, k - 6, FQ)

    def y_send(p, rel):
        ref, n, off = y_buf(p, rel)
        return remote(ref.at[n, pl.ds(BLK, BLK), pl.ds(off, 512)], rc.at[p, 0, :, cols_of[rel]],
                      ys.at[p, rel], yr.at[p, rel], partner)

    def y_zsend(p, rel):
        return remote(rc.at[p, 0, rows(1 - tp, 128), cols_of[rel]], rz.at[p, 0, :, cols_of[rel]],
                      vs.at[p, rel], vr.at[p, rel], zdev)

    def y_group(p, rel):
        ref, n, off = y_buf(p, rel)
        h = (hb, dbb)[p]

        def step(i, carry):
            ref[n, :, pl.ds(pl.multiple_of(off + i * ROWS, 128), ROWS)] = dot(h[...], wd[first_of[rel] + i], NN)
            return carry
        lax.fori_loop(0, 2, step, 0)
        y_send(p, rel).start()

    def add_rows(total, count, base, body):
        def step(i, carry):
            body(pl.ds(pl.multiple_of(base + i * count, count), count), i)
            return carry
        lax.fori_loop(0, total // count, step, 0)

    def y_finish(p, rel):
        ref, n, off = y_buf(p, rel)
        cols = cols_of[rel]
        y_send(p, rel).wait_recv()

        def both(rr, i):
            rc[p, 0, rr, cols] = rc[p, 0, rr, cols] + ref[n, rr, pl.ds(off, 512)]
        add_rows(BLK, 64, 0, both)
        y_zsend(p, rel).start()
        x = (xb, fb)[p]

        def keep(rr, i):
            rc[p, 0, rr, cols] = rc[p, 0, rr, cols] + x[rr, cols].astype(F32)
        add_rows(128, 64, tp * 128, keep)

    def dx_block(p):
        def step(i, carry):
            cols = pl.ds(pl.multiple_of(i * ROWS, ROWS), ROWS)
            pb[p, :, cols] = dot(dab[...], wg[cols, :], NT) + dot(dbb[...], wu[cols, :], NT)
            return carry
        lax.fori_loop(0, 8, step, 0, unroll=2)
        c_send(p).start()

    def c_send(p):
        return remote(pb.at[p, pl.ds(BLK, BLK)], rc.at[p, 1], cs.at[p], cr.at[p], partner)

    def z_send(p):
        return remote(rc.at[p, 1, rows(1 - tp, 128)], rz.at[p, 1], zs.at[p], zr.at[p], zdev)

    def dx_finish(p, dy):
        c_send(p).wait_recv()

        def both(rr, i):
            rc[p, 1, rr, :] = rc[p, 1, rr, :] + pb[p, rr, :]
        add_rows(BLK, 32, 0, both)
        z_send(p).start()

        def keep(rr, i):
            rc[p, 1, rr, :] = rc[p, 1, rr, :] + dy[rr, :].astype(F32)
        add_rows(128, 32, tp * 128, keep)

    outs = (y_out, dx_out)

    def out_rows(p, half):
        return pl.ds(pl.multiple_of(p * BLK + half * 128, 128), 128)

    def fb_at(p, a):
        return fb.at[rows(p * 2 + a, 128)]

    def b_send(p, a):
        return remote(fb_at(p, a), outs[a].at[out_rows(p, tp)], bs.at[p, a], br.at[p, a], zdev)

    def b_local(p, a):
        return pltpu.make_async_copy(fb_at(p, a), outs[a].at[out_rows(p, tp)], fl.at[p, a])

    def finalize(p, a):
        if a == 0:
            for rel in range(4):
                y_zsend(p, rel).wait_recv()
        else:
            z_send(p).wait_recv()

        def body(rr, i):
            kr = pl.ds(pl.multiple_of(tp * 128 + i * 32, 32), 32)
            fr = pl.ds(pl.multiple_of((p * 2 + a) * 128 + i * 32, 32), 32)
            fb[fr, :] = (rc[p, a, kr, :] + rz[p, a, rr, :]).astype(BF16)
        add_rows(128, 32, 0, body)
        b_send(p, a).start()
        b_local(p, a).start()

    on_plane(lambda a: [e_own(a, k).start() for k in BOTH])
    for m in BOTH:
        for c in w_direct(m):
            c.start()
    for m in (0, 1, 2):
        w_local(m).start()
    for p in BOTH:
        for a in BOTH:
            t_partner(a, p).start()
    e_arrived(1)
    e_arrived(2)
    e_crossed(1)
    e_crossed(2)
    for m in BOTH:
        w_wait(m, 1)
        w_wait(m, 4)
        for c in w_forward(m):
            c.start()
    for c in w_direct(2):
        c.start()

    for p in BOTH:
        for a in BOTH:
            t_partner(a, p).wait_recv()
    first_loads = p_loads(0, 0, xb, 0) + p_loads(1, 0, dyb, 1) + p_loads(0, 1, fb, 2)
    for c in first_loads:
        c.start()
    for c in first_loads:
        c.wait()
    everything = pl.ds(0, 2 * BLK)
    transposes(xb, dyb, everything, 2 * BLK)

    for m in BOTH:
        w_local(m).wait()
        for slot in (0, 2, 3, 5, 6):
            w_wait(m, slot)

    def silu_up(a, b):
        return (a * jax.nn.sigmoid(a) * b).astype(BF16)

    def early0(cols):
        a = dot(xb[...], wg[:, cols], NN)
        b = dot(xb[...], wu[:, cols], NN)
        pb[0, :, cols], pb[1, :, cols] = a, b
        hb[:, cols] = silu_up(a, b)
    tiles(early0)
    a, b = rest_pair(xb, everything)
    pb[0, :, rest], pb[1, :, rest] = a, b
    hb[:, rest] = silu_up(a, b)
    w_local(2).wait()
    w_wait(2, 0)
    y_group(0, 0)

    def early1(cols):
        a = dot(fb[...], wg[:, cols], NN)
        b = dot(fb[...], wu[:, cols], NN)
        ab[0, :, cols], ab[1, :, cols] = a, b
        dbb[:, cols] = silu_up(a, b)
    tiles(early1)
    a, b = rest_pair(fb, everything)
    ab[0, :, rest], ab[1, :, rest] = a, b
    dbb[:, rest] = silu_up(a, b)
    y_finish(0, 0)
    y_group(1, 0)

    w_wait(2, 1)
    w_wait(2, 4)
    for c in w_forward(2):
        c.start()
    for j in range(1, PIECES):
        for a in BOTH:
            for k in BOTH:
                t_own(a, j, k).start()
    for a in BOTH:
        t_forward(a, 0).start()
    y_finish(1, 0)
    w_wait(2, 2)
    y_group(0, 1)
    y_group(1, 1)
    w_wait(2, 3)
    y_finish(0, 1)
    y_group(0, 2)
    y_finish(1, 1)
    y_group(1, 2)
    y_finish(0, 2)
    y_finish(1, 2)
    w_wait(2, 5)
    w_wait(2, 6)
    y_group(0, 3)
    y_group(1, 3)

    def late(cols):
        _, dab[:, cols], dbb[:, cols] = gates(pb[0, :, cols], pb[1, :, cols], grad_tile(dyb, everything, cols))
    y_finish(0, 3)
    tiles(late, True)
    late(rest)
    y_finish(1, 3)
    for p in BOTH:
        for rel in range(4):
            y_send(p, rel).wait_send()
    dy1_loads = p_loads(1, 1, xb, 0)
    for c in dy1_loads:
        c.start()
    dx_block(0)
    weight_grads(2 * BLK, first=True)
    dx_finish(0, dyb)
    for c in dy1_loads:
        c.wait()
    transposes(fb, xb, everything, 2 * BLK)

    def late1(cols):
        g = grad_tile(xb, everything, cols)
        hb[:, cols], dab[:, cols], dbb[:, cols] = gates(ab[0, :, cols], ab[1, :, cols], g)
    tiles(late1, True)
    late1(rest)
    dx_block(1)
    finalize(0, 0)
    weight_grads(2 * BLK)
    dx_finish(1, xb)
    finalize(1, 0)

    def unit_of(k):
        diag = k // (2 * PIECES)
        return ((1 - diag) * (1 + lax.rem(k, 2)) + diag * 3,
                (1 - diag) * (k // 2) + diag * (k - 2 * PIECES))

    def service(k):
        rel, j = unit_of(k)
        slot = lax.rem(k, 2)
        for a in BOTH:
            @pl.when(k > 1)
            def _(a=a):
                t_wait_own(a, rel, j)
                t_share(a, rel, j).start()
            u_load(a, rel, j, 0, slot).start()

        @pl.when(jnp.logical_and(k > 1, rel == 1 + core))
        def _():
            for a in BOTH:
                t_forward(a, j).start()

    def other_half(k):
        rel, j = unit_of(k)
        slot = lax.rem(k, 2)
        for a in BOTH:
            t_share(a, rel, j).wait_recv()
            u_load(a, rel, j, 1, slot).start()

    service(jnp.int32(0))
    other_half(jnp.int32(0))
    last = 3 * PIECES - 1

    def unit(k, carry):
        rel, j = unit_of(k)
        slot = lax.rem(k, 2)

        @pl.when(k < last - 1)
        def _():
            service(k + 1)

        for half in BOTH:
            for a in BOTH:
                u_load(a, rel, j, half, slot).wait()
        r = pl.ds(pl.multiple_of(slot * BLK, BLK), BLK)
        phase1(xb, dyb, r, pl.ds(0, BLK), True)
        transposes(xb, dyb, r, BLK)

        @pl.when(k < last - 1)
        def _():
            other_half(k + 1)

        @pl.when(k == last - 1)
        def _():
            service(k + 1)
        weight_grads(BLK, unroll=True)

        @pl.when(k == last - 1)
        def _():
            other_half(k + 1)

        for p in BOTH:
            @pl.when(k == 4 + 3 * p)
            def _():
                finalize(p, 1)
        return carry
    lax.fori_loop(0, 3 * PIECES, unit, 0)

    grads = (dwg_out, dwu_out, dwd_out)

    def g_part(n, c):
        return acc.at[n, pl.ds(pl.multiple_of(c * ROWS, ROWS), ROWS), :]

    def g_at(n):
        return grads[n].at[:, pl.ds(pl.multiple_of(core * FQ, 128), FQ)]

    g_send = [remote(g_part(n, 1 - core), g_at(n), ds.at[n], dr.at[n], partner) for n in range(3)]
    g_local = [pltpu.make_async_copy(g_part(n, core), g_at(n), dl.at[n]) for n in range(3)]
    for n in range(3):
        g_send[n].start()
        g_local[n].start()

    for m in (0, 1, 2):
        for c in w_direct(m) + w_forward(m):
            c.wait_send()
    for a in BOTH:
        for j in range(PIECES):
            if j:
                for k in BOTH:
                    t_own(a, j, k).wait_send()
            t_forward(a, j).wait_send()
            for rel in (1, 2, 3):
                t_share(a, rel, j).wait_send()

    def e_drain(a):
        for k in BOTH:
            e_own(a, k).wait_send()
        for rel in (1, 2):
            e_zshare(a, rel).wait_send()
    on_plane(e_drain)
    for p in BOTH:
        for rel in range(4):
            y_zsend(p, rel).wait_send()
        c_send(p).wait_send()
        z_send(p).wait_send()
        for a in BOTH:
            t_partner(a, p).wait_send()
            b_local(p, a).wait()
            b_send(p, a).wait()
    for n in range(3):
        g_local[n].wait()
        g_send[n].wait()


def write_out(y, dx, g, u, d, y_o, dx_o, g_o, u_o, d_o, yv, dxv, gv, uv, dv, tv, rs, ss):
    loads = [pltpu.make_async_copy(src, dst, rs.at[i])
             for i, (src, dst) in enumerate(((d, dv), (y, yv), (dx, dxv), (g, gv), (u, uv)))]
    stores = [pltpu.make_async_copy(src, dst, ss.at[i])
              for i, (src, dst) in enumerate(((tv, d_o), (yv, y_o), (dxv, dx_o), (gv, g_o), (uv, u_o)))]
    for c in loads:
        c.start()
    loads[0].wait()

    def step(i, carry):
        tv[pl.ds(pl.multiple_of(i * 256, 256), 256), :] = dv[:, pl.ds(pl.multiple_of(i * 256, 256), 256)].T
        return carry
    for i in (1, 2):
        loads[i].wait()
        stores[i].start()
    lax.fori_loop(0, FH // 256, step, 0)
    stores[0].start()
    for i in (3, 4):
        loads[i].wait()
        stores[i].start()
    for c in stores:
        c.wait()


def solution(mesh):
    sds = jax.ShapeDtypeStruct
    dma, vmem = pltpu.SemaphoreType.DMA, pltpu.VMEM

    def device_pass(x, wg, wu, wd, dy):
        anyspec = pl.BlockSpec(memory_space=pl.ANY)
        out = pl.pallas_call(
            kernel,
            out_shape=[sds((TOK, D), BF16), sds((TOK, D), BF16), sds((ROWS, FH), F32), sds((ROWS, FH), F32),
                       sds((ROWS, FH), F32), sds((8, TOK, D), BF16), sds((8, TOK, D), BF16)],
            in_specs=[anyspec] * 5,
            out_specs=[anyspec] * 7,
            scratch_shapes=[
                vmem((D, FQ), BF16), vmem((D, FQ), BF16), vmem((8, FQ, ROWS), BF16),
                vmem((3, 512, FQ), F32),
                vmem((2 * BLK, D), BF16), vmem((2 * BLK, D), BF16),
                vmem((2 * BLK, FQ), BF16), vmem((2 * BLK, FQ), BF16), vmem((2 * BLK, FQ), BF16),
                vmem((2, 2 * BLK, D), F32), vmem((2, 2, BLK, D), F32), vmem((2, 2, 128, D), F32),
                vmem((2 * BLK, D), BF16),
                vmem((512, 2 * BLK), BF16), vmem((512, 2 * BLK), BF16),
                vmem((2, 2 * BLK, FQ), F32),
                dma((3,)), dma((3, 7)), dma((3, 7)),
                dma((8, 2)), dma((2, 2)), dma((2, 2)),
                dma((2,)), dma((3,)), dma((3,)), dma((3,)),
                dma((PIECES, 2, 2)), dma((PIECES, 2)), dma((4, PIECES, 2)), dma((4, PIECES, 2)), dma((4, PIECES, 2)),
                dma((2, 4)), dma((2, 4)), dma((2, 4)), dma((2, 4)),
                dma((2,)), dma((2,)), dma((2,)), dma((2,)), dma((2, 2)), dma((2, 2)), dma((2, 2)),
                dma((3,)), dma((3,)), dma((3,)),
            ],
            compiler_params=pltpu.CompilerParams(collective_id=0, has_side_effects=True,
                                                 vmem_limit_bytes=67043328),
        )(x, wg, wu, wd, dy)
        shapes = [((TOK, D), BF16)] * 2 + [((ROWS, FH), F32)] * 3
        return pl.pallas_call(
            write_out,
            out_shape=[sds(*s) for s in shapes[:4]] + [sds((FH, ROWS), F32)],
            in_specs=[anyspec] * 5,
            out_specs=[anyspec] * 5,
            scratch_shapes=[vmem(*s) for s in shapes] + [vmem((FH, ROWS), F32), dma((5,)), dma((5,))],
            compiler_params=pltpu.CompilerParams(vmem_limit_bytes=67043328),
        )(*out[:5])

    row_spec = P('dp', None)
    weight_spec = P('dp', 'tp')
    down_spec = P('tp', 'dp')
    return jax.shard_map(device_pass, mesh=mesh,
                         in_specs=(row_spec, weight_spec, weight_spec, down_spec, row_spec),
                         out_specs=(row_spec, row_spec, weight_spec, weight_spec, down_spec),
                         check_vma=False)
```

```python
import functools

import jax
import jax.numpy as jnp
from jax import lax
from jax.experimental import pallas as pl
from jax.experimental.pallas import tpu as pltpu
from jax.sharding import PartitionSpec as P

MESH = pl.DeviceIdType.MESH
BOTH = (0, 1)
BF16, F32 = jnp.bfloat16, jnp.float32
D, FH, FQ, ROWS, TOK = 2048, 2816, 1408, 256, 512
SUB, BLK, PIECES = 128, 256, 4
NN = (((1,), (0,)), ((), ()))
NT = (((1,), (1,)), ((), ()))


def dot(a, b, dims):
    return lax.dot_general(a, b, dims, preferred_element_type=F32)


def kernel(x_in, wg_in, wu_in, wd_in, dy_in,
           y_out, dx_out, dwg_out, dwu_out, dwd_out, x_all, dy_all,
           wg, wu, wd, acc, xb, dyb, hb, dab, dbb, pb, rc, rz, fb, xt, dyt, ab,
           wl, ws, wr, xl, os, orr, es, er, ezs, ezr, xs, xf, xd, xr, pr, ys, yr, vs, vr, cs, cr, zs, zr, bs, br, fl, ds, dr, dl):
    tp, dp = lax.axis_index('tp'), lax.axis_index('dp')
    core, xc, yc = lax.rem(dp, 2), lax.rem(lax.div(dp, 2), 2), lax.div(dp, 4)
    col = lax.div(dp, 2)

    def idx(yy, xx, cc):
        return yy * 4 + xx * 2 + cc

    def dev(yy, xx, cc):
        return (tp, idx(yy, xx, cc))

    partner = dev(yc, xc, 1 - core)
    zdev = (1 - tp, dp)

    barrier = pltpu.get_barrier_semaphore()
    peers = [partner, zdev] + [dev(yc, 1 - xc, cc) for cc in BOTH] + [dev(1 - yc, xc, cc) for cc in BOTH]
    for peer in peers:
        pl.semaphore_signal(barrier, inc=1, device_id=peer, device_id_type=MESH)
    pl.semaphore_wait(barrier, len(peers))

    def remote(src, dst, ssem, rsem, device):
        return pltpu.make_async_remote_copy(src_ref=src, dst_ref=dst, send_sem=ssem, recv_sem=rsem,
                                            device_id=device, device_id_type=MESH)

    def w_src(m, cc):
        if m == 2:
            return wd_in.at[pl.ds(pl.multiple_of(cc * FQ, 128), FQ), :]
        return (wg_in, wu_in)[m].at[:, pl.ds(pl.multiple_of(cc * FQ, 128), FQ)]

    def w_at(m, r):
        if m == 2:
            return wd.at[r]
        return (wg, wu)[m].at[pl.ds(pl.multiple_of(r * ROWS, ROWS), ROWS), :]

    def w_local(m):
        return pltpu.make_async_copy(w_src(m, core), w_at(m, dp), wl.at[m])

    def w_direct(m):
        out = [remote(w_src(m, 1 - core), w_at(m, dp), ws.at[m, 0], wr.at[m, 0], partner)]
        for cc in BOTH:
            out.append(remote(w_src(m, cc), w_at(m, dp), ws.at[m, 1 + cc], wr.at[m, 1 + core], dev(yc, 1 - xc, cc)))
            out.append(remote(w_src(m, cc), w_at(m, dp), ws.at[m, 3 + cc], wr.at[m, 3 + core], dev(1 - yc, xc, cc)))
        return out

    rx, ry = idx(yc, 1 - xc, 0), idx(1 - yc, xc, 1)

    def w_forward(m):
        return [remote(w_at(m, rx), w_at(m, rx), ws.at[m, 5], wr.at[m, 5], dev(1 - yc, xc, core)),
                remote(w_at(m, ry), w_at(m, ry), ws.at[m, 6], wr.at[m, 6], dev(yc, 1 - xc, core))]

    def w_wait(m, slot):
        remote(w_at(m, dp), w_at(m, dp), ws.at[m, slot], wr.at[m, slot], partner).wait_recv()

    arrays = ((x_in, x_all), (dy_in, dy_all))

    def rows(j, size=SUB):
        return pl.ds(pl.multiple_of(j * size, size), size)

    def t_at(a, rel, s, j):
        return arrays[a][1].at[rel * 2 + s, rows(j)]

    def t_partner(a, p):
        return remote(arrays[a][0].at[rows(p, BLK)], arrays[a][1].at[core, rows(p, BLK)],
                      os.at[p, a], orr.at[p, a], partner)

    def t_own(a, j, k):
        return remote(arrays[a][0].at[rows(j)], t_at(a, 1 + k, core, j), xs.at[j, a, k], xr.at[1 + k, j, a],
                      (dev(yc, 1 - xc, core), dev(1 - yc, xc, core))[k])

    def t_share(a, rel, j):
        return remote(t_at(a, rel, core, j), t_at(a, rel, core, j), xd.at[rel, j, a], pr.at[rel, j, a], partner)

    fwd_dev = dev(yc + (1 - core) * (1 - 2 * yc), xc + core * (1 - 2 * xc), core)

    def t_forward(a, j):
        return remote(t_at(a, 1 + core, core, j), t_at(a, 3, core, j), xf.at[j, a], xr.at[3, j, a], fwd_dev)

    def t_wait_own(a, rel, j):
        remote(t_at(a, rel, core, j), t_at(a, rel, core, j), xd.at[rel, j, a], xr.at[rel, j, a], partner).wait_recv()

    def p_loads(a, p, ref, sem):
        return [pltpu.make_async_copy(arrays[a][0].at[rows(p, BLK)], ref.at[pl.ds(0, BLK)], xl.at[sem, 0]),
                pltpu.make_async_copy(arrays[a][1].at[1 - core, rows(p, BLK)], ref.at[pl.ds(BLK, BLK)], xl.at[sem, 1])]

    bufs = (xb, dyb)

    def u_load(a, rel, j, half, slot):
        source = core if half == 0 else 1 - core
        return pltpu.make_async_copy(t_at(a, rel, source, j),
                                     bufs[a].at[pl.ds(pl.multiple_of(slot * BLK + half * SUB, SUB), SUB)],
                                     xl.at[4 + slot * 2 + half, a])

    def e_own(a, k):
        return remote(arrays[a][0].at[rows(0)], t_at(a, 1 + k, core, 0), es.at[k], er.at[1 + k],
                      (dev(yc, 1 - xc, core), dev(1 - yc, xc, core))[k])

    def e_zshare(a, rel):
        return remote(t_at(a, rel, core, 0), t_at(a, rel, core, 0), ezs.at[rel], ezr.at[rel], zdev)

    def on_plane(body):
        for a in BOTH:
            @pl.when(tp == a)
            def _(a=a):
                body(a)

    def e_arrived(rel):
        def body(a):
            remote(t_at(a, rel, core, 0), t_at(a, rel, core, 0), ezs.at[rel], er.at[rel], partner).wait_recv()
            e_zshare(a, rel).start()
            t_share(a, rel, 0).start()
        on_plane(body)

    def e_crossed(rel):
        def body(a):
            e_zshare(1 - a, rel).wait_recv()
            t_share(1 - a, rel, 0).start()
        on_plane(body)

    def gates(a, b, g):
        s = jax.nn.sigmoid(a)
        silu = a * s
        return ((silu * b).astype(BF16), (g * b * s * (1.0 + a * (1.0 - s))).astype(BF16), (g * silu).astype(BF16))

    main, rest = FQ // 256, pl.ds(FQ // 256 * 256, FQ % 256)

    def tiles(body, unroll=False):
        def step(n, carry):
            body(pl.ds(pl.multiple_of(n * 256, 256), 256))
            return carry
        lax.fori_loop(0, main, step, 0, unroll=unroll)

    def grad_tile(dy, r, cols):
        g = dot(dy[r, 0:ROWS], wd[0, cols, :], NT)
        for i in range(1, 8):
            g = g + dot(dy[r, i * ROWS:(i + 1) * ROWS], wd[i, cols, :], NT)
        return g

    def rest_pair(x, r):
        both = dot(x[r, :], jnp.concatenate([wg[:, rest], wu[:, rest]], axis=1), NN)
        return both[:, 0:FQ % 256], both[:, FQ % 256:]

    def phase1(x, dy, r, o, unroll=False):
        def body(cols):
            a = dot(x[r, :], wg[:, cols], NN)
            b = dot(x[r, :], wu[:, cols], NN)
            hb[o, cols], dab[o, cols], dbb[o, cols] = gates(a, b, grad_tile(dy, r, cols))
        tiles(body, unroll)
        a, b = rest_pair(x, r)
        hb[o, rest], dab[o, rest], dbb[o, rest] = gates(a, b, grad_tile(dy, r, rest))

    def transposes(x, dy, r, size):
        own_cols = pl.ds(pl.multiple_of(col * 512, 512), 512)
        xt[:, 0:size] = x[r, own_cols].T
        dyt[:, 0:size] = dy[r, own_cols].T

    def weight_grads(size, first=False, unroll=False):
        o = pl.ds(0, size)

        def put(n, cols, value):
            acc[n, :, cols] = value if first else acc[n, :, cols] + value

        def body(cols):
            put(0, cols, dot(xt[:, 0:size], dab[o, cols], NN))
            put(1, cols, dot(xt[:, 0:size], dbb[o, cols], NN))
            put(2, cols, dot(dyt[:, 0:size], hb[o, cols], NN))
        tiles(body, unroll)
        both = dot(xt[:, 0:size], jnp.concatenate([dab[o, rest], dbb[o, rest]], axis=1), NN)
        put(0, rest, both[:, 0:FQ % 256])
        put(1, rest, both[:, FQ % 256:])
        put(2, rest, dot(dyt[:, 0:size], hb[o, rest], NN))

    cols_of = [pl.ds(pl.multiple_of(q * 512, 512), 512)
               for q in (col, yc * 2 + 1 - xc, (1 - yc) * 2 + xc, (1 - yc) * 2 + 1 - xc)]
    first_of = [q * 2 for q in (col, yc * 2 + 1 - xc, (1 - yc) * 2 + xc, (1 - yc) * 2 + 1 - xc)]

    def y_buf(p, rel):
        k = p * 4 + rel
        return (acc, k // 2, k % 2 * 512) if k < 6 else (pb, k - 6, FQ)

    def y_send(p, rel):
        ref, n, off = y_buf(p, rel)
        return remote(ref.at[n, pl.ds(BLK, BLK), pl.ds(off, 512)], rc.at[p, 0, :, cols_of[rel]],
                      ys.at[p, rel], yr.at[p, rel], partner)

    def y_zsend(p, rel):
        return remote(rc.at[p, 0, rows(1 - tp, 128), cols_of[rel]], rz.at[p, 0, :, cols_of[rel]],
                      vs.at[p, rel], vr.at[p, rel], zdev)

    def y_group(p, rel):
        ref, n, off = y_buf(p, rel)
        h = (hb, dbb)[p]

        def step(i, carry):
            ref[n, :, pl.ds(pl.multiple_of(off + i * ROWS, 128), ROWS)] = dot(h[...], wd[first_of[rel] + i], NN)
            return carry
        lax.fori_loop(0, 2, step, 0)
        y_send(p, rel).start()

    def add_rows(total, count, base, body):
        def step(i, carry):
            body(pl.ds(pl.multiple_of(base + i * count, count), count), i)
            return carry
        lax.fori_loop(0, total // count, step, 0)

    def y_finish(p, rel):
        ref, n, off = y_buf(p, rel)
        cols = cols_of[rel]
        y_send(p, rel).wait_recv()

        def both(rr, i):
            rc[p, 0, rr, cols] = rc[p, 0, rr, cols] + ref[n, rr, pl.ds(off, 512)]
        add_rows(BLK, 64, 0, both)
        y_zsend(p, rel).start()
        x = (xb, fb)[p]

        def keep(rr, i):
            rc[p, 0, rr, cols] = rc[p, 0, rr, cols] + x[rr, cols].astype(F32)
        add_rows(128, 64, tp * 128, keep)

    def dx_block(p):
        def step(i, carry):
            cols = pl.ds(pl.multiple_of(i * ROWS, ROWS), ROWS)
            pb[p, :, cols] = dot(dab[...], wg[cols, :], NT) + dot(dbb[...], wu[cols, :], NT)
            return carry
        lax.fori_loop(0, 8, step, 0, unroll=2)
        c_send(p).start()

    def c_send(p):
        return remote(pb.at[p, pl.ds(BLK, BLK)], rc.at[p, 1], cs.at[p], cr.at[p], partner)

    def z_send(p):
        return remote(rc.at[p, 1, rows(1 - tp, 128)], rz.at[p, 1], zs.at[p], zr.at[p], zdev)

    def dx_finish(p, dy):
        c_send(p).wait_recv()

        def both(rr, i):
            rc[p, 1, rr, :] = rc[p, 1, rr, :] + pb[p, rr, :]
        add_rows(BLK, 32, 0, both)
        z_send(p).start()

        def keep(rr, i):
            rc[p, 1, rr, :] = rc[p, 1, rr, :] + dy[rr, :].astype(F32)
        add_rows(128, 32, tp * 128, keep)

    outs = (y_out, dx_out)

    def out_rows(p, half):
        return pl.ds(pl.multiple_of(p * BLK + half * 128, 128), 128)

    def fb_at(p, a):
        return fb.at[rows(p * 2 + a, 128)]

    def b_send(p, a):
        return remote(fb_at(p, a), outs[a].at[out_rows(p, tp)], bs.at[p, a], br.at[p, a], zdev)

    def b_local(p, a):
        return pltpu.make_async_copy(fb_at(p, a), outs[a].at[out_rows(p, tp)], fl.at[p, a])

    def finalize(p, a):
        if a == 0:
            for rel in range(4):
                y_zsend(p, rel).wait_recv()
        else:
            z_send(p).wait_recv()

        def body(rr, i):
            kr = pl.ds(pl.multiple_of(tp * 128 + i * 32, 32), 32)
            fr = pl.ds(pl.multiple_of((p * 2 + a) * 128 + i * 32, 32), 32)
            fb[fr, :] = (rc[p, a, kr, :] + rz[p, a, rr, :]).astype(BF16)
        add_rows(128, 32, 0, body)
        b_send(p, a).start()
        b_local(p, a).start()

    on_plane(lambda a: [e_own(a, k).start() for k in BOTH])
    for m in BOTH:
        for c in w_direct(m):
            c.start()
    for m in (0, 1, 2):
        w_local(m).start()
    for p in BOTH:
        for a in BOTH:
            t_partner(a, p).start()
    e_arrived(1)
    e_arrived(2)
    e_crossed(1)
    e_crossed(2)
    for m in BOTH:
        w_wait(m, 1)
        w_wait(m, 4)
        for c in w_forward(m):
            c.start()
    for c in w_direct(2):
        c.start()

    for p in BOTH:
        for a in BOTH:
            t_partner(a, p).wait_recv()
    first_loads = p_loads(0, 0, xb, 0) + p_loads(1, 0, dyb, 1) + p_loads(0, 1, fb, 2)
    for c in first_loads:
        c.start()
    for c in first_loads:
        c.wait()
    everything = pl.ds(0, 2 * BLK)
    transposes(xb, dyb, everything, 2 * BLK)

    for m in BOTH:
        w_local(m).wait()
        for slot in (0, 2, 3, 5, 6):
            w_wait(m, slot)

    def silu_up(a, b):
        return (a * jax.nn.sigmoid(a) * b).astype(BF16)

    def early0(cols):
        a = dot(xb[...], wg[:, cols], NN)
        b = dot(xb[...], wu[:, cols], NN)
        pb[0, :, cols], pb[1, :, cols] = a, b
        hb[:, cols] = silu_up(a, b)
    tiles(early0)
    a, b = rest_pair(xb, everything)
    pb[0, :, rest], pb[1, :, rest] = a, b
    hb[:, rest] = silu_up(a, b)
    w_local(2).wait()
    w_wait(2, 0)
    y_group(0, 0)

    def early1(cols):
        a = dot(fb[...], wg[:, cols], NN)
        b = dot(fb[...], wu[:, cols], NN)
        ab[0, :, cols], ab[1, :, cols] = a, b
        dbb[:, cols] = silu_up(a, b)
    tiles(early1)
    a, b = rest_pair(fb, everything)
    ab[0, :, rest], ab[1, :, rest] = a, b
    dbb[:, rest] = silu_up(a, b)
    y_finish(0, 0)
    y_group(1, 0)

    w_wait(2, 1)
    w_wait(2, 4)
    for c in w_forward(2):
        c.start()
    for j in range(1, PIECES):
        for a in BOTH:
            for k in BOTH:
                t_own(a, j, k).start()
    for a in BOTH:
        t_forward(a, 0).start()
    y_finish(1, 0)
    w_wait(2, 2)
    y_group(0, 1)
    y_group(1, 1)
    w_wait(2, 3)
    y_finish(0, 1)
    y_group(0, 2)
    y_finish(1, 1)
    y_group(1, 2)
    y_finish(0, 2)
    y_finish(1, 2)
    w_wait(2, 5)
    w_wait(2, 6)
    y_group(0, 3)
    y_group(1, 3)

    def late(cols):
        _, dab[:, cols], dbb[:, cols] = gates(pb[0, :, cols], pb[1, :, cols], grad_tile(dyb, everything, cols))
    y_finish(0, 3)
    tiles(late, True)
    late(rest)
    y_finish(1, 3)
    for p in BOTH:
        for rel in range(4):
            y_send(p, rel).wait_send()
    dy1_loads = p_loads(1, 1, xb, 0)
    for c in dy1_loads:
        c.start()
    dx_block(0)
    weight_grads(2 * BLK, first=True)
    dx_finish(0, dyb)
    for c in dy1_loads:
        c.wait()
    transposes(fb, xb, everything, 2 * BLK)

    def late1(cols):
        g = grad_tile(xb, everything, cols)
        hb[:, cols], dab[:, cols], dbb[:, cols] = gates(ab[0, :, cols], ab[1, :, cols], g)
    tiles(late1, True)
    late1(rest)
    dx_block(1)
    finalize(0, 0)
    weight_grads(2 * BLK)
    dx_finish(1, xb)
    finalize(1, 0)

    def unit_of(k):
        diag = k // (2 * PIECES)
        return ((1 - diag) * (1 + lax.rem(k, 2)) + diag * 3,
                (1 - diag) * (k // 2) + diag * (k - 2 * PIECES))

    def service(k):
        rel, j = unit_of(k)
        slot = lax.rem(k, 2)
        for a in BOTH:
            @pl.when(k > 1)
            def _(a=a):
                t_wait_own(a, rel, j)
                t_share(a, rel, j).start()
            u_load(a, rel, j, 0, slot).start()

        @pl.when(jnp.logical_and(k > 1, rel == 1 + core))
        def _():
            for a in BOTH:
                t_forward(a, j).start()

    def other_half(k):
        rel, j = unit_of(k)
        slot = lax.rem(k, 2)
        for a in BOTH:
            t_share(a, rel, j).wait_recv()
            u_load(a, rel, j, 1, slot).start()

    service(jnp.int32(0))
    other_half(jnp.int32(0))
    last = 3 * PIECES - 1

    def unit(k, carry):
        rel, j = unit_of(k)
        slot = lax.rem(k, 2)

        @pl.when(k < last - 1)
        def _():
            service(k + 1)

        for half in BOTH:
            for a in BOTH:
                u_load(a, rel, j, half, slot).wait()
        r = pl.ds(pl.multiple_of(slot * BLK, BLK), BLK)
        phase1(xb, dyb, r, pl.ds(0, BLK), True)
        transposes(xb, dyb, r, BLK)

        @pl.when(k < last - 1)
        def _():
            other_half(k + 1)

        @pl.when(k == last - 1)
        def _():
            service(k + 1)
        weight_grads(BLK, unroll=True)

        @pl.when(k == last - 1)
        def _():
            other_half(k + 1)

        for p in BOTH:
            @pl.when(k == 4 + 3 * p)
            def _():
                finalize(p, 1)
        return carry
    lax.fori_loop(0, 3 * PIECES, unit, 0)

    grads = (dwg_out, dwu_out, dwd_out)

    def g_part(n, c):
        return acc.at[n, pl.ds(pl.multiple_of(c * ROWS, ROWS), ROWS), :]

    def g_at(n):
        return grads[n].at[:, pl.ds(pl.multiple_of(core * FQ, 128), FQ)]

    g_send = [remote(g_part(n, 1 - core), g_at(n), ds.at[n], dr.at[n], partner) for n in range(3)]
    g_local = [pltpu.make_async_copy(g_part(n, core), g_at(n), dl.at[n]) for n in range(3)]
    for n in range(3):
        g_send[n].start()
        g_local[n].start()

    for m in (0, 1, 2):
        for c in w_direct(m) + w_forward(m):
            c.wait_send()
    for a in BOTH:
        for j in range(PIECES):
            if j:
                for k in BOTH:
                    t_own(a, j, k).wait_send()
            t_forward(a, j).wait_send()
            for rel in (1, 2, 3):
                t_share(a, rel, j).wait_send()

    def e_drain(a):
        for k in BOTH:
            e_own(a, k).wait_send()
        for rel in (1, 2):
            e_zshare(a, rel).wait_send()
    on_plane(e_drain)
    for p in BOTH:
        for rel in range(4):
            y_zsend(p, rel).wait_send()
        c_send(p).wait_send()
        z_send(p).wait_send()
        for a in BOTH:
            t_partner(a, p).wait_send()
            b_local(p, a).wait()
            b_send(p, a).wait()
    for n in range(3):
        g_local[n].wait()
        g_send[n].wait()


def write_out(y, dx, g, u, d, y_o, dx_o, g_o, u_o, d_o, yv, dxv, gv, uv, dv, tv, rs, ss, ts):
    loads = [pltpu.make_async_copy(src, dst, rs.at[i])
             for i, (src, dst) in enumerate(((d, dv), (y, yv), (dx, dxv), (g, gv), (u, uv)))]
    stores = [pltpu.make_async_copy(src, dst, ss.at[i])
              for i, (src, dst) in enumerate(((yv, y_o), (dxv, dx_o), (gv, g_o), (uv, u_o)))]
    def tile_store(i):
        part = pl.ds(pl.multiple_of(i * 256, 256), 256)
        return pltpu.make_async_copy(tv.at[part], d_o.at[part], ts.at[i])

    def step(i, carry):
        part = pl.ds(pl.multiple_of(i * 256, 256), 256)
        tv[part, :] = dv[:, part].T
        tile_store(i).start()
        return carry

    def done(i, carry):
        tile_store(i).wait()
        return carry

    for c in loads:
        c.start()
    loads[0].wait()
    lax.fori_loop(0, FH // 256, step, 0)
    for load, store in zip(loads[1:], stores):
        load.wait()
        store.start()
    lax.fori_loop(0, FH // 256, done, 0)
    for c in stores:
        c.wait()


def solution(mesh):
    sds = jax.ShapeDtypeStruct
    dma, vmem = pltpu.SemaphoreType.DMA, pltpu.VMEM

    def device_pass(x, wg, wu, wd, dy):
        anyspec = pl.BlockSpec(memory_space=pl.ANY)
        out = pl.pallas_call(
            kernel,
            out_shape=[sds((TOK, D), BF16), sds((TOK, D), BF16), sds((ROWS, FH), F32), sds((ROWS, FH), F32),
                       sds((ROWS, FH), F32), sds((8, TOK, D), BF16), sds((8, TOK, D), BF16)],
            in_specs=[anyspec] * 5,
            out_specs=[anyspec] * 7,
            scratch_shapes=[
                vmem((D, FQ), BF16), vmem((D, FQ), BF16), vmem((8, FQ, ROWS), BF16),
                vmem((3, 512, FQ), F32),
                vmem((2 * BLK, D), BF16), vmem((2 * BLK, D), BF16),
                vmem((2 * BLK, FQ), BF16), vmem((2 * BLK, FQ), BF16), vmem((2 * BLK, FQ), BF16),
                vmem((2, 2 * BLK, D), F32), vmem((2, 2, BLK, D), F32), vmem((2, 2, 128, D), F32),
                vmem((2 * BLK, D), BF16),
                vmem((512, 2 * BLK), BF16), vmem((512, 2 * BLK), BF16),
                vmem((2, 2 * BLK, FQ), F32),
                dma((3,)), dma((3, 7)), dma((3, 7)),
                dma((8, 2)), dma((2, 2)), dma((2, 2)),
                dma((2,)), dma((3,)), dma((3,)), dma((3,)),
                dma((PIECES, 2, 2)), dma((PIECES, 2)), dma((4, PIECES, 2)), dma((4, PIECES, 2)), dma((4, PIECES, 2)),
                dma((2, 4)), dma((2, 4)), dma((2, 4)), dma((2, 4)),
                dma((2,)), dma((2,)), dma((2,)), dma((2,)), dma((2, 2)), dma((2, 2)), dma((2, 2)),
                dma((3,)), dma((3,)), dma((3,)),
            ],
            compiler_params=pltpu.CompilerParams(collective_id=0, has_side_effects=True,
                                                 vmem_limit_bytes=67043328),
        )(x, wg, wu, wd, dy)
        shapes = [((TOK, D), BF16)] * 2 + [((ROWS, FH), F32)] * 3
        return pl.pallas_call(
            write_out,
            out_shape=[sds(*s) for s in shapes[:4]] + [sds((FH, ROWS), F32)],
            in_specs=[anyspec] * 5,
            out_specs=[anyspec] * 5,
            scratch_shapes=[vmem(*s) for s in shapes] + [vmem((FH, ROWS), F32), dma((5,)), dma((4,)), dma((FH // 256,))],
            compiler_params=pltpu.CompilerParams(vmem_limit_bytes=67043328),
        )(*out[:5])

    row_spec = P('dp', None)
    weight_spec = P('dp', 'tp')
    down_spec = P('tp', 'dp')
    return jax.shard_map(device_pass, mesh=mesh,
                         in_specs=(row_spec, weight_spec, weight_spec, down_spec, row_spec),
                         out_specs=(row_spec, row_spec, weight_spec, weight_spec, down_spec),
                         check_vma=False)
```
